512 devices in a mesh: parts: 2 (over y), tm: 32 (over z), sub: 4 (over x), inner: 2 (over core).
Axes of the slice: x: 4, y: 2, z: 32, core: 2. Of those that a mesh axis runs over, the one named last changes fastest.
The devices are a block of a 4x16x32 slice.
Arguments:
- guess: float32 [8192, 128], P(('parts', 'tm', 'sub', 'inner')), parts along dimension 0, may hold values from -6 to 6
- start: float32 [256], P('parts'), parts along dimension 0, may hold values from -6 to 6
- layer_weight: float32 [256, 64], replicated, may hold values from -0.75 to 0.75
- layer_bias: float32 [256], replicated, may hold values from -4 to 4
- amplitude: float32 [256], replicated, may hold values from 0.5 to 4
Outputs:
- updated: float32 [8192, 128], P(('parts', 'tm', 'sub', 'inner')), parts along dimension 0
The draws below stay inside these ranges and needn't reach their ends.
There are 2 independent parts, one for each index of `parts`. The reference program is written for one: setup_inputs(seed, part) draws one part's arguments, and reference() takes and returns one part's arrays. A program takes and returns all parts, laid end to end along the dimension named above; an argument that names none is the same for every part. Nothing has to cross between parts.
All inputs are finite; a program needn't handle non-finite values.
Results may differ from the reference program's by a relative error of at most 0.0003.
Values sent between devices are 32-bit elements; how exact they have to be, the bound alone decides.
A program may use at most 128 MiB of HBM per device.

```python
import math
import jax
import jax.numpy as jnp
from jax import lax

COORD = 64
HIDDEN_SIZE = 256
STATE = 128
STEPS = 4096


def block_levels(key, dims, cuts, low, top_value):
    level, own = 1.0, jax.random.fold_in(key, 6)
    for dim, shards_of in cuts:
        steps = jnp.exp(jax.random.uniform(jax.random.fold_in(own, dim), (shards_of,), jnp.float32, low / len(cuts), top_value / len(cuts)))
        level = level * jnp.repeat(steps, dims[dim] // shards_of).reshape([-1 if axis == dim else 1 for axis in range(len(dims))])
    return level


def gaussian(key, shape, deviation, most, split=(), kind=jnp.bfloat16):
    values = deviation * jax.random.normal(key, shape, jnp.float32)
    if split:
        values = values * block_levels(key, shape, split, -0.22, 0.18)
    return jnp.clip(values, -most, most).astype(kind)


def setup_inputs(seed: int = 0, part: int = 0) -> dict:
    key_of = jax.random.split(jax.random.key(seed), 6)
    part_splits = jax.random.split(jax.random.fold_in(key_of[5], part), 6)
    guess = gaussian(part_splits[0], (STEPS, STATE), 1.0, 6.0, ((0, 256),), jnp.float32)
    start = gaussian(part_splits[1], (STATE,), 1.0, 6.0, (), jnp.float32)
    layer_weight = gaussian(key_of[2], (HIDDEN_SIZE, COORD), COORD ** -0.5, 0.75, (), jnp.float32)
    layer_bias = gaussian(key_of[3], (HIDDEN_SIZE,), 1.0, 4.0, (), jnp.float32)
    amplitude = jnp.clip(jnp.exp(jax.random.uniform(key_of[4], (HIDDEN_SIZE,), jnp.float32, math.log(0.5), math.log(4.0))), 0.5, 4.0)
    return dict(guess=guess, start=start, layer_weight=layer_weight, layer_bias=layer_bias, amplitude=amplitude)


step_size = 0.04
curvature = 0.5


def forces(coords, layer_weight, layer_bias, amplitude):
    hi = lax.Precision.HIGHEST
    pre = jnp.dot(coords, layer_weight.T, precision=hi) + layer_bias
    gate = jax.nn.sigmoid(pre)
    grad = jnp.dot(amplitude * gate, layer_weight, precision=hi) + curvature * coords
    return grad, amplitude * gate * (1.0 - gate)


def hess_apply(vector, layer_weight, weights_d):
    hi = lax.Precision.HIGHEST
    inner_vals = jnp.dot(layer_weight, vector, precision=hi) * weights_d
    return jnp.dot(inner_vals, layer_weight, precision=hi) + curvature * vector


def reference(guess, start, layer_weight, layer_bias, amplitude):
    width = layer_weight.shape[1]
    before = jnp.concatenate([start[None, :], guess[:-1]], axis=0)
    coords, momenta = before[:, :width], before[:, width:]
    grad_zero, curve_zero = forces(coords, layer_weight, layer_bias, amplitude)
    half = momenta - 0.5 * step_size * grad_zero
    moved = coords + step_size * half
    grad_one, curve_one = forces(moved, layer_weight, layer_bias, amplitude)
    landed = half - 0.5 * step_size * grad_one
    image = jnp.concatenate([moved, landed], axis=1)

    def advance(state, items):
        prior, curve_a, curve_b, target = items
        delta = state - prior
        delta_q, delta_p = delta[:width], delta[width:]
        first = hess_apply(delta_q, layer_weight, curve_a)
        new_q = delta_q - 0.5 * step_size * step_size * first + step_size * delta_p
        new_p = delta_p - 0.5 * step_size * first - 0.5 * step_size * hess_apply(new_q, layer_weight, curve_b)
        result = target + jnp.concatenate([new_q, new_p])
        return result, result

    final, states = lax.scan(advance, start, (before, curve_zero, curve_one, image))
    return states
```

```python
import functools

import jax
import jax.numpy as jnp
from jax import lax
from jax.experimental import pallas as pl
from jax.experimental.pallas import tpu as pltpu
from jax.sharding import PartitionSpec as P

step_size = 0.04
curvature = 0.5
half_step = 0.5 * step_size
f32, bf16 = jnp.float32, jnp.bfloat16
MESH = pl.DeviceIdType.MESH
planes = 4
tail = 8


def iota(shape, axis):
    return lax.broadcasted_iota(jnp.int32, shape, axis)


def split(value):
    high = value.astype(bf16)
    return high, (value - high.astype(f32)).astype(bf16)


def low_lanes(value):
    width = value.shape[-1]
    return iota(value.shape, 1) < width // 2


def mixed(value):
    high = value.astype(bf16).astype(f32)
    return jnp.where(low_lanes(value), high, value - high).astype(bf16)


def twice(value):
    swapped = pltpu.roll(value, value.shape[-1] // 2, 1)
    low = low_lanes(value)
    return jnp.where(low, value, swapped), jnp.where(low, swapped, value)


def join(coords, momenta):
    return jnp.where(low_lanes(coords), coords, momenta)


def dot(left, right):
    return jnp.dot(left, right, preferred_element_type=f32)


def with_tail(value, extra):
    rows = value.shape[0] - tail
    return jnp.concatenate([value[:rows], value[rows:] + extra], axis=0)


def compose(first, second):
    state = first.shape[1]
    eye = (iota((state, state), 0) == iota((state, state), 1)).astype(f32)
    high, low = split(second[:state] - eye)
    both = jnp.concatenate([high, low], axis=1)
    left = jnp.concatenate(split(first), axis=1)
    out = dot(left, jnp.concatenate([both, both], axis=0))
    return with_tail(first + (out[:, :state] + out[:, state:]), second[state:])


def chain(maps):
    while len(maps) > 1:
        maps = [
            compose(maps[k], maps[k + 1]) if k + 1 < len(maps) else maps[k]
            for k in range(0, len(maps), 2)
        ]
    return maps[0]


def identity(state):
    rows = state + tail
    return (iota((rows, state), 0) == iota((rows, state), 1)).astype(f32)


def applied(vector, full):
    state = vector.shape[1]
    eye = iota((state, state), 0) == iota((state, state), 1)
    column = jnp.sum(jnp.where(eye, vector, 0.0), axis=1, keepdims=True)
    return jnp.sum(column * full[:state], axis=0, keepdims=True) + full[state : state + 1]


class Local:
    def __init__(self, guess, start, weight, bias, amplitude):
        self.steps, self.state = guess.shape
        steps = self.steps
        doubled = jnp.concatenate([weight, weight], axis=1)
        self.across = doubled.T
        high, low = split(self.across)
        self.onto = jnp.concatenate([high, low], axis=0)
        high, low = split(doubled)
        self.back = jnp.concatenate([high, low], axis=1)
        self.width = self.state // 2
        rows = jnp.concatenate([guess, jnp.broadcast_to(start, (tail, self.state))], axis=0)
        coords, momenta = twice(rows)
        grad_zero, curve_zero = self.forces(coords, bias, amplitude)
        half = momenta - half_step * grad_zero
        moved = coords + step_size * half
        grad_one, curve_one = self.forces(moved, bias, amplitude)
        landed = half - half_step * grad_one
        self.first = join(moved, landed)[steps : steps + 1]
        coords, momenta = coords[:steps], momenta[:steps]
        self.curve_zero, self.curve_one = curve_zero[:steps], curve_one[:steps]
        self.moved, self.landed = moved[:steps], landed[:steps]
        self.start_q, self.start_p = coords[:1], momenta[:1]
        inside = iota((steps, 1), 0) < steps - 1

        def later(value):
            return jnp.where(inside, pltpu.roll(value, steps - 1, 0), 0.0)

        self.curve_next = later(self.curve_zero)
        self.off_q = self.moved - later(coords)
        off_p = self.landed - later(momenta)
        pulled = jnp.where(inside, self.off_q, 0.0)
        kicked = self.apart(self.along(pulled) * self.curve_next) + curvature * pulled
        self.off_p = off_p - half_step * kicked

    def along(self, value):
        left = mixed(value)
        return dot(jnp.concatenate([left, left], axis=1), self.onto)

    def apart(self, value):
        state = self.state
        high, low = split(value)
        out = dot(high, self.back) + dot(low, self.back)
        return out[:, :state] + out[:, state:]

    def forces(self, coords, bias, amplitude):
        gate = 1.0 / (1.0 + jnp.exp(-(self.along(coords) + bias)))
        pull = amplitude * gate
        return self.apart(pull) + curvature * coords, pull * (1.0 - gate)

    def hessians(self, curves, diagonal):
        count = curves.shape[0]
        width, state = self.width, self.state
        across = self.across[:width]
        scaled = [across * curves[k : k + 1] for k in range(count)]
        parts = [split(value) for value in scaled]
        stacked = jnp.concatenate([p[0] for p in parts] + [p[1] for p in parts], axis=0)
        out = dot(stacked, self.back)
        out = out[:, :state] + out[:, state:]
        out = out[: count * width] + out[count * width :]
        unit = jnp.where(iota((width, state), 0) == iota((width, state), 1) % width, 1.0, 0.0)
        found = []
        for k in range(count):
            high, low = split(out[k * width : (k + 1) * width] + diagonal[k] * unit)
            found.append(jnp.concatenate([high, high, low, low], axis=0))
        return found


def kick(coords, kicks):
    left = mixed(coords)
    return half_step * dot(jnp.concatenate([left, left], axis=1), kicks)


def window_map(local, kicks, opening):
    steps, state = local.steps, local.state
    runs = 4
    length = steps // runs
    ident = identity(state)
    maps = []
    states = []
    for c in range(runs):
        coords, momenta = twice(ident)
        if c == 0:
            coords, momenta = with_tail(coords, -local.start_q), with_tail(momenta, -local.start_p)
            momenta = momenta - kick(coords, opening)
        states.append((coords, momenta))
    for j in range(length):
        for c in range(runs):
            t = c * length + j
            coords, momenta = states[c]
            coords = coords + step_size * momenta
            momenta = momenta - kick(coords, kicks[t])
            states[c] = (
                with_tail(coords, local.off_q[t : t + 1]),
                with_tail(momenta, local.off_p[t : t + 1]),
            )
    return chain([join(*s) for s in states])


def kernel(
    sizes, guess_ref, start_ref, weight_ref, bias_ref, amplitude_ref, out_ref,
    kicks_ref, open_ref, offs_ref, rows_ref, core_ref, subs_ref, majors_ref, groups_ref,
    pre_ref, run_ref, vector_ref, spread_ref,
    core_sems, subs_send, subs_recv, majors_send, majors_recv, groups_send, groups_recv,
    pre_sems, spread_send, vector_recv, tokens,
):
    n_tm, n_sub, n_inner = sizes
    n_groups = n_tm // planes
    part, tm = lax.axis_index("parts"), lax.axis_index("tm")
    sub, inner = lax.axis_index("sub"), lax.axis_index("inner")
    group, plane = lax.div(tm, planes), lax.rem(tm, planes)
    middle = planes // 2
    state = guess_ref.shape[1]
    steps = guess_ref.shape[0]
    last = n_inner - 1
    lead = inner == last
    head = jnp.logical_and(lead, plane == middle)
    serves = jnp.logical_and(head, lax.rem(group, n_sub) == sub)
    serving_sub = lax.rem(group, n_sub)

    def place(tm_at=None, sub_at=None, inner_at=None):
        return (
            part,
            tm if tm_at is None else tm_at,
            sub if sub_at is None else sub_at,
            inner if inner_at is None else inner_at,
        )

    barrier = pltpu.get_barrier_semaphore()

    def greet(where):
        pl.semaphore_signal(barrier, inc=1, device_id=where, device_id_type=MESH)

    group_up = lax.rem(group + 1, n_groups) * planes + middle
    group_down = lax.rem(group + n_groups - 1, n_groups) * planes + middle

    greet(place(inner_at=n_inner - 1 - inner))

    @pl.when(jnp.logical_not(serves))
    def _():
        greet(place(group * planes + middle, serving_sub, last))

    @pl.when(lead)
    def _():
        for k in range(1, n_sub):
            greet(place(sub_at=lax.rem(sub + k, n_sub)))

    @pl.when(head)
    def _():
        for k in range(1, planes):
            greet(place(group * planes + lax.rem(middle + k, planes)))
        greet(place(group_up))
        greet(place(group_down))

    local = Local(
        guess_ref[...], start_ref[...], weight_ref[...], bias_ref[...], amplitude_ref[...]
    )
    diagonal = [2.0 * curvature] * (steps - 1) + [curvature, curvature]
    curves = jnp.concatenate(
        [local.curve_one + local.curve_next, jnp.broadcast_to(local.curve_zero[:1], (tail, local.curve_zero.shape[1]))],
        axis=0,
    )[: steps + 1]
    found = local.hessians(curves, diagonal)
    window = window_map(local, found[:steps], found[steps])
    own_ref = run_ref
    own_ref[...] = window

    for t in range(steps):
        kicks_ref[t, :, :state] = found[t]
    open_ref[...] = found[steps]
    offs_ref[0] = local.off_q
    offs_ref[1] = local.off_p
    rows_ref[0] = local.moved
    rows_ref[1] = local.landed
    first = local.first
    start_q, start_p = local.start_q, local.start_p

    count = jnp.where(lead, n_sub, 1) + jnp.where(lead, jnp.where(head, 2, 1), 0)
    count = count + jnp.where(serves, planes * n_sub * n_inner - 1, 0)
    pl.semaphore_wait(barrier, count)

    rounds = list(range(2, n_groups // 2 + 1))

    def tell(r):
        for where in (place(group_up), place(group_down)):
            pl.semaphore_signal(tokens.at[r - 2], inc=1, device_id=where, device_id_type=MESH)

    def hear(position):
        if position < len(rounds):
            pl.semaphore_wait(tokens.at[rounds[position] - 2], 2)
            if position + 1 < len(rounds):
                tell(rounds[position + 1])

    def copy(source, target, send, recv, where):
        return pltpu.make_async_remote_copy(
            src_ref=source, dst_ref=target, send_sem=send, recv_sem=recv,
            device_id=where, device_id_type=MESH,
        )

    if rounds:
        @pl.when(head)
        def _():
            tell(rounds[0])

    to_lead = copy(own_ref, core_ref, core_sems.at[0], core_sems.at[1], place(inner_at=last))

    @pl.when(jnp.logical_not(lead))
    def _():
        to_lead.start()

    @pl.when(lead)
    def _():
        to_lead.wait_recv()
        subs_ref[sub] = compose(core_ref[...], own_ref[...])
        for k in range(1, n_sub):
            copy(
                subs_ref.at[sub], subs_ref.at[sub], subs_send.at[k - 1], subs_recv.at[sub],
                place(sub_at=lax.rem(sub + k, n_sub)),
            ).start()

        @pl.when(head)
        def _():
            hear(0)

        for k in range(1, n_sub):
            other = lax.rem(sub + k, n_sub)
            copy(
                subs_ref.at[other], subs_ref.at[other], subs_send.at[k - 1], subs_recv.at[other],
                place(sub_at=other),
            ).wait_recv()
        majors_ref[plane] = chain([subs_ref[k] for k in range(n_sub)])

        @pl.when(jnp.logical_not(head))
        def _():
            copy(
                majors_ref.at[plane], majors_ref.at[plane], majors_send, majors_recv.at[plane],
                place(group * planes + middle),
            ).start()

        @pl.when(head)
        def _():
            hear(1)
            for k in range(planes):
                if k != middle:
                    copy(
                        majors_ref.at[k], majors_ref.at[k], majors_send, majors_recv.at[k],
                        place(group * planes + k),
                    ).wait_recv()
            groups_ref[group] = chain([majors_ref[k] for k in range(planes)])
            for position in range(2, max(3, len(rounds))):
                hear(position)
            for m in range(-(-n_groups // n_sub)):
                to = m * n_sub + sub

                @pl.when(jnp.logical_and(to > group, to < n_groups))
                def _():
                    copy(
                        groups_ref.at[group], groups_ref.at[group], groups_send.at[m],
                        groups_recv.at[group], place(to * planes + middle),
                    ).start()

        pre_ref[...] = identity(state)
        for k in range(n_sub - 1):
            @pl.when(k < sub)
            def _():
                pre_ref[...] = compose(pre_ref[...], subs_ref[k])

    to_other = copy(pre_ref, pre_ref, pre_sems.at[0], pre_sems.at[1], place(inner_at=0))

    @pl.when(lead)
    def _():
        to_other.start()

    @pl.when(jnp.logical_not(lead))
    def _():
        to_lead.wait_send()
        to_other.wait_recv()
        own_ref[...] = pre_ref[...]

    @pl.when(lead)
    def _():
        own_ref[...] = compose(pre_ref[...], core_ref[...])

    plain = local.hessians(local.curve_one, [curvature] * steps)
    for t in range(steps):
        kicks_ref[t, :, state:] = plain[t]

    coords, momenta = twice(own_ref[...])
    coords, momenta = with_tail(coords, -start_q), with_tail(momenta, -start_p)
    momenta = momenta - kick(coords, open_ref[...])
    maps_ref = spread_ref

    def advance(t, carry):
        coords, momenta = carry
        coords = coords + step_size * momenta
        both = kick(coords, kicks_ref[t])
        row = pl.ds(t, 1)
        maps_ref[t] = join(
            with_tail(coords, rows_ref[0, row, :]),
            with_tail(momenta - both[:, state:], rows_ref[1, row, :]),
        )
        return (
            with_tail(coords, offs_ref[0, row, :]),
            with_tail(momenta - both[:, :state], offs_ref[1, row, :]),
        )

    lax.fori_loop(0, steps - 1, advance, (coords, momenta))

    @pl.when(serves)
    def _():
        vector_ref[0] = jnp.broadcast_to(first, (tail, state))
        for k in range(n_groups - 1):
            @pl.when(k < group)
            def _():
                copy(
                    groups_ref.at[k], groups_ref.at[k], groups_send.at[0], groups_recv.at[k],
                    place(k * planes + middle),
                ).wait_recv()
                vector_ref[0] = jnp.broadcast_to(
                    applied(vector_ref[0, :1, :], groups_ref[k]), (tail, state)
                )
        entering = [vector_ref[0, :1, :]]
        for k in range(planes - 1):
            entering.append(applied(entering[-1], majors_ref[k]))
        for k in range(planes):
            vector_ref[1 + k] = jnp.broadcast_to(entering[k], (tail, state))

    def to_each(act):
        for k in range(planes):
            for s in range(n_sub):
                for c in range(n_inner):
                    at = (k * n_sub + s) * n_inner + c

                    def go(k=k, s=s, c=c, at=at):
                        act(copy(
                            vector_ref.at[1 + k], vector_ref.at[1 + planes],
                            spread_send_sems.at[at], vector_recv,
                            place(group * planes + k, s, c),
                        ))

                    if k == middle and c == last:
                        pl.when(s != sub)(go)
                    else:
                        go()

    spread_send_sems = spread_send

    @pl.when(serves)
    def _():
        to_each(lambda c: c.start())
        vector_ref[1 + planes] = vector_ref[1 + middle]

    @pl.when(jnp.logical_not(serves))
    def _():
        copy(
            vector_ref.at[1], vector_ref.at[1 + planes], spread_send.at[0], vector_recv,
            place(group * planes + middle, serving_sub, last),
        ).wait_recv()

    vector = vector_ref[1 + planes, :1, :]
    eye = iota((state, state), 0) == iota((state, state), 1)
    column = jnp.sum(jnp.where(eye, vector, 0.0), axis=1, keepdims=True)
    for t in range(steps):
        ref = own_ref if t == 0 else maps_ref.at[t - 1]
        out_ref[t : t + 1, :] = (
            jnp.sum(column * ref[:state, :], axis=0, keepdims=True) + ref[state : state + 1, :]
        )

    @pl.when(lead)
    def _():
        for k in range(1, n_sub):
            copy(
                subs_ref.at[sub], subs_ref.at[sub], subs_send.at[k - 1], subs_recv.at[sub],
                place(sub_at=lax.rem(sub + k, n_sub)),
            ).wait_send()
        to_other.wait_send()

        @pl.when(jnp.logical_not(head))
        def _():
            copy(
                majors_ref.at[plane], majors_ref.at[plane], majors_send, majors_recv.at[plane],
                place(group * planes + middle),
            ).wait_send()

        @pl.when(head)
        def _():
            for m in range(-(-n_groups // n_sub)):
                to = m * n_sub + sub

                @pl.when(jnp.logical_and(to > group, to < n_groups))
                def _():
                    copy(
                        groups_ref.at[group], groups_ref.at[group], groups_send.at[m],
                        groups_recv.at[group], place(to * planes + middle),
                    ).wait_send()

    @pl.when(serves)
    def _():
        to_each(lambda c: c.wait_send())


def shards(sizes, guess, start, layer_weight, layer_bias, amplitude):
    n_tm, n_sub, n_inner = sizes
    steps, state = guess.shape
    rows = state + tail
    n_groups = n_tm // planes
    vmem = pl.BlockSpec(memory_space=pltpu.VMEM)
    dma, regular = pltpu.SemaphoreType.DMA, pltpu.SemaphoreType.REGULAR
    return pl.pallas_call(
        functools.partial(kernel, sizes),
        out_shape=jax.ShapeDtypeStruct((steps, state), f32),
        in_specs=[vmem] * 5,
        out_specs=vmem,
        scratch_shapes=[
            pltpu.VMEM((steps, 2 * state, 2 * state), bf16),
            pltpu.VMEM((2 * state, state), bf16),
            pltpu.VMEM((2, steps, state), f32),
            pltpu.VMEM((2, steps, state), f32),
            pltpu.VMEM((rows, state), f32),
            pltpu.VMEM((n_sub, rows, state), f32),
            pltpu.VMEM((planes, rows, state), f32),
            pltpu.VMEM((n_groups, rows, state), f32),
            pltpu.VMEM((rows, state), f32),
            pltpu.VMEM((rows, state), f32),
            pltpu.VMEM((2 + planes, tail, state), f32),
            pltpu.VMEM((steps, rows, state), f32),
            dma((2,)),
            dma((n_sub,)),
            dma((n_sub,)),
            dma,
            dma((planes,)),
            dma((-(-n_groups // n_sub),)),
            dma((n_groups,)),
            dma((2,)),
            dma((planes * n_sub * n_inner,)),
            dma,
            regular((max(1, n_groups // 2),)),
        ],
        compiler_params=pltpu.CompilerParams(collective_id=0, has_side_effects=True),
    )(guess, start.reshape(1, -1), layer_weight, layer_bias.reshape(1, -1), amplitude.reshape(1, -1))


def solution(mesh):
    sizes = tuple(mesh.shape[name] for name in ("tm", "sub", "inner"))
    placed = (P(("parts", "tm", "sub", "inner"), None), P("parts"), P(), P(), P())
    return jax.shard_map(
        functools.partial(shards, sizes),
        mesh=mesh,
        in_specs=placed,
        out_specs=P(("parts", "tm", "sub", "inner"), None),
        check_vma=False,
    )
```

```python
import functools

import jax
import jax.numpy as jnp
from jax import lax
from jax.experimental import pallas as pl
from jax.experimental.pallas import tpu as pltpu
from jax.sharding import PartitionSpec as P

step_size = 0.04
curvature = 0.5
half_step = 0.5 * step_size
f32, bf16 = jnp.float32, jnp.bfloat16
MESH = pl.DeviceIdType.MESH
planes = 4
tail = 8


def iota(shape, axis):
    return lax.broadcasted_iota(jnp.int32, shape, axis)


def split(value):
    high = value.astype(bf16)
    return high, (value - high.astype(f32)).astype(bf16)


def low_lanes(value):
    width = value.shape[-1]
    return iota(value.shape, 1) < width // 2


def mixed(value):
    high = value.astype(bf16).astype(f32)
    return jnp.where(low_lanes(value), high, value - high).astype(bf16)


def twice(value):
    swapped = pltpu.roll(value, value.shape[-1] // 2, 1)
    low = low_lanes(value)
    return jnp.where(low, value, swapped), jnp.where(low, swapped, value)


def join(coords, momenta):
    return jnp.where(low_lanes(coords), coords, momenta)


def dot(left, right):
    return jnp.dot(left, right, preferred_element_type=f32)


def with_tail(value, extra):
    rows = value.shape[0] - tail
    return jnp.concatenate([value[:rows], value[rows:] + extra], axis=0)


def compose(first, second):
    state = first.shape[1]
    eye = (iota((state, state), 0) == iota((state, state), 1)).astype(f32)
    high, low = split(second[:state] - eye)
    both = jnp.concatenate([high, low], axis=1)
    left = jnp.concatenate(split(first), axis=1)
    out = dot(left, jnp.concatenate([both, both], axis=0))
    return with_tail(first + (out[:, :state] + out[:, state:]), second[state:])


def chain(maps):
    while len(maps) > 1:
        maps = [
            compose(maps[k], maps[k + 1]) if k + 1 < len(maps) else maps[k]
            for k in range(0, len(maps), 2)
        ]
    return maps[0]


def identity(state):
    rows = state + tail
    return (iota((rows, state), 0) == iota((rows, state), 1)).astype(f32)


def applied(vector, full):
    state = vector.shape[1]
    eye = iota((state, state), 0) == iota((state, state), 1)
    column = jnp.sum(jnp.where(eye, vector, 0.0), axis=1, keepdims=True)
    return jnp.sum(column * full[:state], axis=0, keepdims=True) + full[state : state + 1]


class Local:
    def __init__(self, guess, start, weight, bias, amplitude):
        self.steps, self.state = guess.shape
        steps = self.steps
        self.across = jnp.concatenate([weight, weight], axis=0)
        doubled = self.across.T
        high, low = split(self.across)
        self.onto = jnp.concatenate([high, low], axis=0)
        high, low = split(doubled)
        self.back = jnp.concatenate([high, low], axis=1)
        self.width = self.state // 2
        rows = jnp.concatenate([guess, jnp.broadcast_to(start, (tail, self.state))], axis=0)
        coords, momenta = twice(rows)
        grad_zero, curve_zero = self.forces(coords, bias, amplitude)
        half = momenta - half_step * grad_zero
        moved = coords + step_size * half
        grad_one, curve_one = self.forces(moved, bias, amplitude)
        landed = half - half_step * grad_one
        self.first = join(moved, landed)[steps : steps + 1]
        coords, momenta = coords[:steps], momenta[:steps]
        self.curve_zero, self.curve_one = curve_zero[:steps], curve_one[:steps]
        self.moved, self.landed = moved[:steps], landed[:steps]
        self.start_q, self.start_p = coords[:1], momenta[:1]
        inside = iota((steps, 1), 0) < steps - 1

        def later(value):
            return jnp.where(inside, pltpu.roll(value, steps - 1, 0), 0.0)

        self.curve_next = later(self.curve_zero)
        self.off_q = self.moved - later(coords)
        off_p = self.landed - later(momenta)
        pulled = jnp.where(inside, self.off_q, 0.0)
        kicked = self.apart(self.along(pulled) * self.curve_next) + curvature * pulled
        self.off_p = off_p - half_step * kicked

    def along(self, value):
        left = mixed(value)
        return dot(jnp.concatenate([left, left], axis=1), self.onto)

    def apart(self, value):
        state = self.state
        high, low = split(value)
        out = dot(high, self.back) + dot(low, self.back)
        return out[:, :state] + out[:, state:]

    def forces(self, coords, bias, amplitude):
        gate = 1.0 / (1.0 + jnp.exp(-(self.along(coords) + bias)))
        pull = amplitude * gate
        return self.apart(pull) + curvature * coords, pull * (1.0 - gate)

    def hessians(self, curves, diagonal):
        count = curves.shape[0]
        width, state = self.width, self.state
        across = self.across[:width]
        scaled = [across * curves[k : k + 1] for k in range(count)]
        parts = [split(value) for value in scaled]
        stacked = jnp.concatenate([p[0] for p in parts] + [p[1] for p in parts], axis=0)
        out = dot(stacked, self.back)
        out = out[:, :state] + out[:, state:]
        out = out[: count * width] + out[count * width :]
        unit = jnp.where(iota((width, state), 0) == iota((width, state), 1) % width, 1.0, 0.0)
        found = []
        for k in range(count):
            high, low = split(out[k * width : (k + 1) * width] + diagonal[k] * unit)
            found.append(jnp.concatenate([high, high, low, low], axis=0))
        return found


def kick(coords, kicks):
    left = mixed(coords)
    return half_step * dot(jnp.concatenate([left, left], axis=1), kicks)


def window_map(local, kicks, opening):
    steps, state = local.steps, local.state
    runs = 4
    length = steps // runs
    ident = identity(state)
    maps = []
    states = []
    for c in range(runs):
        coords, momenta = twice(ident)
        if c == 0:
            coords, momenta = with_tail(coords, -local.start_q), with_tail(momenta, -local.start_p)
            momenta = momenta - kick(coords, opening)
        states.append((coords, momenta))
    for j in range(length):
        for c in range(runs):
            t = c * length + j
            coords, momenta = states[c]
            coords = coords + step_size * momenta
            momenta = momenta - kick(coords, kicks[t])
            states[c] = (
                with_tail(coords, local.off_q[t : t + 1]),
                with_tail(momenta, local.off_p[t : t + 1]),
            )
    return chain([join(*s) for s in states])


def kernel(
    sizes, guess_ref, start_ref, weight_ref, bias_ref, amplitude_ref, out_ref,
    kicks_ref, open_ref, offs_ref, rows_ref, core_ref, subs_ref, majors_ref, ahead_ref,
    pre_ref, run_ref, vector_ref, maps_ref,
    core_sems, subs_send, subs_recv, majors_send, majors_recv, pre_sems,
    spread_send, vector_recv, entry_send, entry_recv,
):
    n_tm, n_sub, n_inner = sizes
    n_groups = n_tm // planes
    part, tm = lax.axis_index("parts"), lax.axis_index("tm")
    sub, inner = lax.axis_index("sub"), lax.axis_index("inner")
    group, plane = lax.div(tm, planes), lax.rem(tm, planes)
    steps, state = guess_ref.shape
    last = n_inner - 1
    lead = inner == last
    other = jnp.logical_not(lead)
    column = jnp.logical_and(lead, sub == 0)
    head = jnp.logical_and(column, plane == 0)
    opening_chip = jnp.logical_and(tm == 0, sub == 0)
    origin = jnp.logical_and(opening_chip, inner == 0)

    def place(tm_at=None, sub_at=None, inner_at=None):
        return (
            part,
            tm if tm_at is None else tm_at,
            sub if sub_at is None else sub_at,
            inner if inner_at is None else inner_at,
        )

    def copy(source, target, send, recv, where):
        return pltpu.make_async_remote_copy(
            src_ref=source, dst_ref=target, send_sem=send, recv_sem=recv,
            device_id=where, device_id_type=MESH,
        )

    def both(*conditions):
        return functools.reduce(jnp.logical_and, conditions)

    barrier = pltpu.get_barrier_semaphore()

    def greet(where):
        pl.semaphore_signal(barrier, inc=1, device_id=where, device_id_type=MESH)

    @pl.when(jnp.logical_not(origin))
    def _():
        @pl.when(jnp.logical_not(both(opening_chip, lead)))
        def _():
            greet(place(inner_at=n_inner - 1 - inner))

        @pl.when(tm == 0)
        def _():
            greet(place(0, 0, 0))

        @pl.when(both(tm > 0, jnp.logical_not(head)))
        def _():
            greet(place(group * planes, 0, last))

    def takes_from(s):
        return both(lead, sub != s, jnp.logical_or(sub > s, sub == 0))

    def gives_to(t):
        return both(lead, sub != t, jnp.logical_or(sub < t, t == 0))

    for s in range(n_sub):
        @pl.when(takes_from(s))
        def _():
            greet(place(sub_at=s))

    @pl.when(head)
    def _():
        for k in range(1, planes):
            greet(place(group * planes + k))

        @pl.when(group > 0)
        def _():
            greet(place((group - 1) * planes))

    local = Local(
        guess_ref[...], start_ref[...], weight_ref[...], bias_ref[...], amplitude_ref[...]
    )
    diagonal = [2.0 * curvature] * (steps - 1) + [curvature, curvature]
    curves = jnp.concatenate(
        [
            local.curve_one + local.curve_next,
            jnp.broadcast_to(local.curve_zero[:1], (tail, local.curve_zero.shape[1])),
        ],
        axis=0,
    )[: steps + 1]
    found = local.hessians(curves, diagonal)
    run_ref[...] = window_map(local, found[:steps], found[steps])
    first = local.first
    start_q, start_p = local.start_q, local.start_p

    count = jnp.where(jnp.logical_and(lead, jnp.logical_not(opening_chip)), 1, 0)
    count = count + jnp.where(other, 1, 0)
    count = count + jnp.where(lead, jnp.where(sub == 0, n_sub - 1, n_sub - sub), 0)
    count = count + jnp.where(jnp.logical_and(column, plane > 0), 1, 0)
    around = n_sub * n_inner
    count = count + jnp.where(head, (planes - 1) * around, 0)
    count = count + jnp.where(jnp.logical_and(head, group > 0), around - 1, 0)
    count = count + jnp.where(jnp.logical_and(head, group < n_groups - 1), 1, 0)
    count = jnp.where(origin, around - 1, count)
    pl.semaphore_wait(barrier, count)

    entry, arrived, onward = 0, planes + 1, planes + 2
    entering = vector_ref.at[entry]

    def from_origin(act):
        for s in range(n_sub):
            for c in range(n_inner):
                if (s, c) == (0, 0):
                    continue
                ahead = (s, c) == (0, last)
                act(copy(
                    vector_ref.at[onward],
                    entering if ahead else vector_ref.at[arrived],
                    spread_send.at[s * n_inner + c],
                    entry_recv if ahead else vector_recv,
                    place(0, s, c),
                ))

    @pl.when(origin)
    def _():
        vector_ref[onward] = jnp.broadcast_to(applied(first, run_ref), (tail, state))
        from_origin(lambda c: c.start())
        vector_ref[arrived] = jnp.broadcast_to(first, (tail, state))

    for t in range(steps):
        kicks_ref[t, :, :state] = found[t]
    open_ref[...] = found[steps]
    offs_ref[0] = local.off_q
    offs_ref[1] = local.off_p
    rows_ref[0] = local.moved
    rows_ref[1] = local.landed
    plain = local.hessians(local.curve_one, [curvature] * steps)
    for t in range(steps):
        kicks_ref[t, :, state:] = plain[t]

    to_lead = copy(run_ref, core_ref, core_sems.at[0], core_sems.at[1], place(inner_at=last))
    to_other = copy(pre_ref, pre_ref, pre_sems.at[0], pre_sems.at[1], place(inner_at=0))
    to_head = copy(
        majors_ref.at[plane], majors_ref.at[plane], majors_send, majors_recv.at[plane],
        place(group * planes),
    )

    def to_sub(t):
        return copy(
            subs_ref.at[sub], subs_ref.at[sub], subs_send.at[t], subs_recv.at[sub],
            place(sub_at=t),
        )

    @pl.when(jnp.logical_and(other, jnp.logical_not(origin)))
    def _():
        to_lead.start()

    @pl.when(lead)
    def _():
        @pl.when(opening_chip)
        def _():
            subs_ref[sub] = run_ref[...]

        @pl.when(jnp.logical_not(opening_chip))
        def _():
            to_lead.wait_recv()
            subs_ref[sub] = compose(core_ref[...], run_ref[...])

        for t in range(n_sub):
            @pl.when(gives_to(t))
            def _():
                to_sub(t).start()

        for s in range(n_sub):
            @pl.when(takes_from(s))
            def _():
                copy(
                    subs_ref.at[s], subs_ref.at[s], subs_send.at[s], subs_recv.at[s],
                    place(sub_at=s),
                ).wait_recv()

        pre_ref[...] = identity(state)
        for k in range(n_sub - 1):
            @pl.when(k < sub)
            def _():
                pre_ref[...] = compose(pre_ref[...], subs_ref[k])

        @pl.when(jnp.logical_not(opening_chip))
        def _():
            to_other.start()
            run_ref[...] = compose(pre_ref[...], core_ref[...])

        @pl.when(opening_chip)
        def _():
            run_ref[...] = identity(state)

        @pl.when(sub == 0)
        def _():
            majors_ref[plane] = chain([subs_ref[k] for k in range(n_sub)])

            @pl.when(plane > 0)
            def _():
                to_head.start()

            @pl.when(plane == 0)
            def _():
                ahead_ref[0] = majors_ref[0]
                for k in range(1, planes):
                    copy(
                        majors_ref.at[k], majors_ref.at[k], majors_send, majors_recv.at[k],
                        place(group * planes + k),
                    ).wait_recv()
                    ahead_ref[k] = compose(ahead_ref[k - 1], majors_ref[k])

    @pl.when(other)
    def _():
        @pl.when(origin)
        def _():
            run_ref[...] = identity(state)

        @pl.when(jnp.logical_not(origin))
        def _():
            to_lead.wait_send()
            to_other.wait_recv()
            run_ref[...] = pre_ref[...]

    coords, momenta = twice(run_ref[...])
    coords, momenta = with_tail(coords, -start_q), with_tail(momenta, -start_p)
    momenta = momenta - kick(coords, open_ref[...])

    def advance(t, carry):
        coords, momenta = carry
        coords = coords + step_size * momenta
        pair = kick(coords, kicks_ref[t])
        row = pl.ds(t, 1)
        maps_ref[t] = join(
            with_tail(coords, rows_ref[0, row, :]),
            with_tail(momenta - pair[:, state:], rows_ref[1, row, :]),
        )
        return (
            with_tail(coords, offs_ref[0, row, :]),
            with_tail(momenta - pair[:, :state], offs_ref[1, row, :]),
        )

    lax.fori_loop(0, steps - 1, advance, (coords, momenta))

    def to_next(source):
        return copy(source, entering, entry_send, entry_recv, place((group + 1) * planes))

    def to_each(act):
        def send(k, s, c):
            act(copy(
                entering if k == 0 else vector_ref.at[k],
                vector_ref.at[arrived],
                spread_send.at[(k * n_sub + s) * n_inner + c],
                vector_recv,
                place(group * planes + k, s, c),
            ))

        for k in range(1, planes):
            for s in range(n_sub):
                for c in range(n_inner):
                    send(k, s, c)

        @pl.when(group > 0)
        def _():
            for s in range(n_sub):
                for c in range(n_inner):
                    if (s, c) != (0, last):
                        send(0, s, c)

    @pl.when(head)
    def _():
        to_next(vector_ref.at[onward]).wait_recv()
        here = vector_ref[entry, :1, :]
        for k in range(planes):
            slot = k + 1 if k + 1 < planes else onward
            vector_ref[slot] = jnp.broadcast_to(applied(here, ahead_ref[k]), (tail, state))
        to_each(lambda c: c.start())

        @pl.when(group < n_groups - 1)
        def _():
            to_next(vector_ref.at[onward]).start()

        vector_ref[arrived] = vector_ref[entry]

    @pl.when(both(jnp.logical_not(head), jnp.logical_not(origin)))
    def _():
        copy(
            vector_ref.at[entry], vector_ref.at[arrived], spread_send.at[0], vector_recv,
            place(group * planes, 0, last),
        ).wait_recv()

    vector = vector_ref[arrived, :1, :]
    eye = iota((state, state), 0) == iota((state, state), 1)
    upright = jnp.sum(jnp.where(eye, vector, 0.0), axis=1, keepdims=True)
    for t in range(steps):
        ref = run_ref if t == 0 else maps_ref.at[t - 1]
        out_ref[t : t + 1, :] = (
            jnp.sum(upright * ref[:state, :], axis=0, keepdims=True) + ref[state : state + 1, :]
        )

    @pl.when(origin)
    def _():
        from_origin(lambda c: c.wait_send())

    @pl.when(lead)
    def _():
        for t in range(n_sub):
            @pl.when(gives_to(t))
            def _():
                to_sub(t).wait_send()

        @pl.when(jnp.logical_not(opening_chip))
        def _():
            to_other.wait_send()

        @pl.when(jnp.logical_and(column, plane > 0))
        def _():
            to_head.wait_send()

    @pl.when(head)
    def _():
        to_each(lambda c: c.wait_send())

        @pl.when(group < n_groups - 1)
        def _():
            to_next(vector_ref.at[onward]).wait_send()


def shards(sizes, guess, start, layer_weight, layer_bias, amplitude):
    n_tm, n_sub, n_inner = sizes
    steps, state = guess.shape
    rows = state + tail
    vmem = pl.BlockSpec(memory_space=pltpu.VMEM)
    dma, regular = pltpu.SemaphoreType.DMA, pltpu.SemaphoreType.REGULAR
    return pl.pallas_call(
        functools.partial(kernel, sizes),
        out_shape=jax.ShapeDtypeStruct((steps, state), f32),
        in_specs=[vmem] * 5,
        out_specs=vmem,
        scratch_shapes=[
            pltpu.VMEM((steps, 2 * state, 2 * state), bf16),
            pltpu.VMEM((2 * state, state), bf16),
            pltpu.VMEM((2, steps, state), f32),
            pltpu.VMEM((2, steps, state), f32),
            pltpu.VMEM((rows, state), f32),
            pltpu.VMEM((n_sub, rows, state), f32),
            pltpu.VMEM((planes, rows, state), f32),
            pltpu.VMEM((planes, rows, state), f32),
            pltpu.VMEM((rows, state), f32),
            pltpu.VMEM((rows, state), f32),
            pltpu.VMEM((3 + planes, tail, state), f32),
            pltpu.VMEM((steps, rows, state), f32),
            dma((2,)),
            dma((n_sub,)),
            dma((n_sub,)),
            dma,
            dma((planes,)),
            dma((2,)),
            dma((planes * n_sub * n_inner,)),
            dma,
            dma,
            dma,
        ],
        compiler_params=pltpu.CompilerParams(collective_id=0, has_side_effects=True),
    )(guess, start.reshape(1, -1), layer_weight.T, layer_bias.reshape(1, -1), amplitude.reshape(1, -1))


def solution(mesh):
    sizes = tuple(mesh.shape[name] for name in ("tm", "sub", "inner"))
    placed = (P(("parts", "tm", "sub", "inner"), None), P("parts"), P(), P(), P())
    return jax.shard_map(
        functools.partial(shards, sizes),
        mesh=mesh,
        in_specs=placed,
        out_specs=P(("parts", "tm", "sub", "inner"), None),
        check_vma=False,
    )
```

```python
import functools

import jax
import jax.numpy as jnp
from jax import lax
from jax.experimental import pallas as pl
from jax.experimental.pallas import tpu as pltpu
from jax.sharding import PartitionSpec as P

step_size = 0.04
curvature = 0.5
half_step = 0.5 * step_size
f32, bf16 = jnp.float32, jnp.bfloat16
MESH = pl.DeviceIdType.MESH
planes = 4
tail = 8


def iota(shape, axis):
    return lax.broadcasted_iota(jnp.int32, shape, axis)


def split(value):
    high = value.astype(bf16)
    return high, (value - high.astype(f32)).astype(bf16)


def low_lanes(value):
    width = value.shape[-1]
    return iota(value.shape, 1) < width // 2


def mixed(value):
    high = value.astype(bf16).astype(f32)
    return jnp.where(low_lanes(value), high, value - high).astype(bf16)


def twice(value):
    swapped = pltpu.roll(value, value.shape[-1] // 2, 1)
    low = low_lanes(value)
    return jnp.where(low, value, swapped), jnp.where(low, swapped, value)


def join(coords, momenta):
    return jnp.where(low_lanes(coords), coords, momenta)


def dot(left, right):
    return jnp.dot(left, right, preferred_element_type=f32)


def with_tail(value, extra):
    rows = value.shape[0] - tail
    if rows == 0:
        return value + extra
    return jnp.concatenate([value[:rows], value[rows:] + extra], axis=0)


def compose(first, second):
    state = first.shape[1]
    eye = (iota((state, state), 0) == iota((state, state), 1)).astype(f32)
    high, low = split(second[:state] - eye)
    both = jnp.concatenate([high, low], axis=1)
    left = jnp.concatenate(split(first), axis=1)
    out = dot(left, jnp.concatenate([both, both], axis=0))
    return with_tail(first + (out[:, :state] + out[:, state:]), second[state:])


def chain(maps):
    while len(maps) > 1:
        maps = [
            compose(maps[k], maps[k + 1]) if k + 1 < len(maps) else maps[k]
            for k in range(0, len(maps), 2)
        ]
    return maps[0]


def identity(state):
    rows = state + tail
    return (iota((rows, state), 0) == iota((rows, state), 1)).astype(f32)


def applied(vector, full):
    state = vector.shape[1]
    eye = iota((state, state), 0) == iota((state, state), 1)
    column = jnp.sum(jnp.where(eye, vector, 0.0), axis=1, keepdims=True)
    return jnp.sum(column * full[:state], axis=0, keepdims=True) + full[state : state + 1]


class Weights:
    def __init__(self, across_ref, onto_ref, back_ref, bias_ref, amplitude_ref):
        self.across_ref, self.onto_ref, self.back_ref = across_ref, onto_ref, back_ref
        self.bias_ref, self.amplitude_ref = bias_ref, amplitude_ref

    def fill(self, weight):
        across = jnp.concatenate([weight, weight], axis=0)
        high, low = split(across)
        self.onto_ref[...] = jnp.concatenate([high, low], axis=0)
        high, low = split(across.T)
        self.back_ref[...] = jnp.concatenate([high, low], axis=1)

    def along(self, value):
        left = mixed(value)
        return dot(jnp.concatenate([left, left], axis=1), self.onto_ref[...])

    def apart(self, value):
        back = self.back_ref[...]
        state = back.shape[1] // 2
        high, low = split(value)
        out = dot(high, back) + dot(low, back)
        return out[:, :state] + out[:, state:]

    def forces(self, coords):
        gate = 1.0 / (1.0 + jnp.exp(-(self.along(coords) + self.bias_ref[...])))
        pull = self.amplitude_ref[...] * gate
        return self.apart(pull) + curvature * coords, pull * (1.0 - gate)

    def hessians(self, curves, diagonal):
        count = curves.shape[0]
        across, back = self.across_ref[...], self.back_ref[...]
        width, state = across.shape[0], back.shape[1] // 2
        parts = [split(across * curves[k : k + 1]) for k in range(count)]
        stacked = jnp.concatenate([p[0] for p in parts] + [p[1] for p in parts], axis=0)
        out = dot(stacked, back)
        out = out[:, :state] + out[:, state:]
        out = out[: count * width] + out[count * width :]
        unit = jnp.where(iota((width, state), 0) == iota((width, state), 1) % width, 1.0, 0.0)
        return [out[k * width : (k + 1) * width] + diagonal[k] * unit for k in range(count)]


def stationary(hessian):
    high, low = split(hessian)
    return jnp.concatenate([high, high, low, low], axis=0)


class Window:
    def __init__(self, weights, rows, start):
        self.steps, self.state = steps, state = rows.shape
        coords, momenta = twice(
            jnp.concatenate([rows, jnp.broadcast_to(start, (tail, state))], axis=0)
        )
        grad_zero, curve_zero = weights.forces(coords)
        half = momenta - half_step * grad_zero
        moved = coords + step_size * half
        grad_one, curve_one = weights.forces(moved)
        landed = half - half_step * grad_one
        self.first_q, self.first_p = moved[steps:], landed[steps:]
        self.first = join(self.first_q, self.first_p)[:1]
        coords, momenta = coords[:steps], momenta[:steps]
        self.curve_zero, self.curve_one = curve_zero[:steps], curve_one[:steps]
        self.moved, self.landed = moved[:steps], landed[:steps]
        self.start_q, self.start_p = coords[:1], momenta[:1]
        inside = iota((steps, 1), 0) < steps - 1

        def later(value):
            return jnp.where(inside, pltpu.roll(value, steps - 1, 0), 0.0)

        curve_next = later(self.curve_zero)
        opening = jnp.broadcast_to(self.curve_zero[:1], (tail, self.curve_zero.shape[1]))
        self.curves = jnp.concatenate([self.curve_one + curve_next, opening], axis=0)[: steps + 1]
        self.diagonal = [2.0 * curvature] * (steps - 1) + [curvature, curvature]
        self.off_q = self.moved - later(coords)
        begin_q = self.first_q - self.start_q
        begin_p = self.first_p - self.start_p
        pulled = jnp.concatenate([jnp.where(inside, self.off_q, 0.0), begin_q], axis=0)
        curve = jnp.concatenate([curve_next, opening], axis=0)
        kicked = half_step * (weights.apart(weights.along(pulled) * curve) + curvature * pulled)
        self.off_p = self.landed - later(momenta) - kicked[:steps]
        self.begin_q, self.begin_p = begin_q, begin_p - kicked[steps:]


def kick(coords, kicks):
    left = mixed(coords)
    return half_step * dot(jnp.concatenate([left, left], axis=1), kicks)


def window_map(window, kicks):
    steps, state = window.steps, window.state
    runs = 4
    length = steps // runs
    ident = identity(state)
    states = []
    for c in range(runs):
        coords, momenta = twice(ident)
        if c == 0:
            coords = with_tail(coords, -window.start_q)
            momenta = with_tail(momenta, -window.start_p)
            momenta = momenta - kick(coords, kicks[steps])
        states.append((coords, momenta))
    for j in range(length):
        for c in range(runs):
            t = c * length + j
            coords, momenta = states[c]
            coords = coords + step_size * momenta
            momenta = momenta - kick(coords, kicks[t])
            states[c] = (
                with_tail(coords, window.off_q[t : t + 1]),
                with_tail(momenta, window.off_p[t : t + 1]),
            )
    return chain([join(*s) for s in states])


def left_state(weights, rows, start):
    window = Window(weights, rows, start)
    steps, state = window.steps, window.state
    width = state // 2
    runs = 4
    length = steps // runs
    hessians = weights.hessians(window.curves, window.diagonal)
    repeated = jnp.where(iota((width, state), 0) == iota((width, state), 1) % width, 1.0, 0.0)
    none = jnp.zeros((tail, state), f32)
    moving = jnp.concatenate([repeated, step_size * repeated, none], axis=0)
    states = [(window.begin_q, window.begin_p)]
    for c in range(1, runs):
        t = c * length
        bend = half_step * hessians[t]
        momenta = jnp.concatenate([-bend, repeated - step_size * bend, none], axis=0)
        states.append((
            with_tail(moving, window.off_q[t : t + 1]),
            with_tail(momenta, window.off_p[t : t + 1]),
        ))
    for j in range(length):
        for c in range(runs):
            if j == length - 1 and c > 0:
                continue
            t = c * length + j + (1 if c else 0)
            coords, momenta = states[c]
            coords = coords + step_size * momenta
            momenta = momenta - kick(coords, stationary(hessians[t]))
            states[c] = (
                with_tail(coords, window.off_q[t : t + 1]),
                with_tail(momenta, window.off_p[t : t + 1]),
            )
    maps = [join(*s) for s in states]
    vector = maps[0][:1]
    for full in maps[1:]:
        vector = applied(vector, full)
    return vector


def kernel(
    sizes, guess_hbm, start_hbm, weight_hbm, bias_hbm, amplitude_hbm, out_ref,
    guess_ref, start_ref, weight_ref, bias_ref, amplitude_ref,
    kicks_ref, open_ref, offs_ref, rows_ref, core_ref, subs_ref, majors_ref, ahead_ref,
    pre_ref, run_ref, vector_ref, maps_ref, onto_ref, back_ref, raw_ref,
    core_sems, subs_send, subs_recv, majors_send, majors_recv, pre_sems,
    spread_send, vector_recv, entry_send, entry_recv, raw_recv, load_sems,
):
    n_tm, n_sub, n_inner = sizes
    n_groups = n_tm // planes
    part, tm = lax.axis_index("parts"), lax.axis_index("tm")
    sub, inner = lax.axis_index("sub"), lax.axis_index("inner")
    group, plane = lax.div(tm, planes), lax.rem(tm, planes)
    steps, state = guess_ref.shape
    last = n_inner - 1
    lead = inner == last
    other = jnp.logical_not(lead)
    column = jnp.logical_and(lead, sub == 0)
    head = jnp.logical_and(column, plane == 0)
    opening_chip = jnp.logical_and(tm == 0, sub == 0)
    origin = jnp.logical_and(opening_chip, inner == 0)

    def place(tm_at=None, sub_at=None, inner_at=None):
        return (
            part,
            tm if tm_at is None else tm_at,
            sub if sub_at is None else sub_at,
            inner if inner_at is None else inner_at,
        )

    def copy(source, target, send, recv, where):
        return pltpu.make_async_remote_copy(
            src_ref=source, dst_ref=target, send_sem=send, recv_sem=recv,
            device_id=where, device_id_type=MESH,
        )

    def both(*conditions):
        return functools.reduce(jnp.logical_and, conditions)

    barrier = pltpu.get_barrier_semaphore()
    around = n_sub * n_inner
    loads = [
        pltpu.make_async_copy(source, target, load_sems.at[k])
        for k, (source, target) in enumerate((
            (guess_hbm, guess_ref), (weight_hbm, weight_ref), (start_hbm, start_ref),
            (bias_hbm, bias_ref), (amplitude_hbm, amplitude_ref),
        ))
    ]
    for load in loads:
        load.start()

    def from_origin(act):
        def send(at, carry):
            act(copy(
                guess_ref, raw_ref, spread_send.at[at], raw_recv,
                place(0, lax.div(at, n_inner), lax.rem(at, n_inner)),
            ))
            return carry

        lax.fori_loop(1, around, send, 0)

    @pl.when(origin)
    def _():
        pl.semaphore_wait(barrier, around - 1)
        loads[0].wait()
        from_origin(lambda c: c.start())

    @pl.when(jnp.logical_not(origin))
    def _():
        loads[0].wait()

    def greet(where):
        pl.semaphore_signal(barrier, inc=1, device_id=where, device_id_type=MESH)

    @pl.when(jnp.logical_not(origin))
    def _():
        @pl.when(jnp.logical_not(both(opening_chip, lead)))
        def _():
            greet(place(inner_at=n_inner - 1 - inner))

        @pl.when(tm == 0)
        def _():
            greet(place(0, 0, 0))

        @pl.when(both(tm > 0, jnp.logical_not(head)))
        def _():
            greet(place(group * planes, 0, last))

    def takes_from(s):
        return both(lead, sub != s, jnp.logical_or(sub > s, sub == 0))

    def gives_to(t):
        return both(lead, sub != t, jnp.logical_or(sub < t, t == 0))

    for s in range(n_sub):
        @pl.when(takes_from(s))
        def _():
            greet(place(sub_at=s))

    @pl.when(head)
    def _():
        for k in range(1, planes):
            greet(place(group * planes + k))

        @pl.when(group > 0)
        def _():
            greet(place((group - 1) * planes))

    for load in loads[1:]:
        load.wait()
    weights = Weights(weight_ref, onto_ref, back_ref, bias_ref, amplitude_ref)
    weights.fill(weight_ref[...])
    start = start_ref[...]
    window = Window(weights, guess_ref[...], start)
    found = [stationary(k) for k in weights.hessians(window.curves, window.diagonal)]
    run_ref[...] = window_map(window, found)
    start_q, start_p = window.start_q, window.start_p

    count = jnp.where(jnp.logical_and(lead, jnp.logical_not(opening_chip)), 1, 0)
    count = count + jnp.where(other, 1, 0)
    count = count + jnp.where(lead, jnp.where(sub == 0, n_sub - 1, n_sub - sub), 0)
    count = count + jnp.where(jnp.logical_and(column, plane > 0), 1, 0)
    count = count + jnp.where(head, (planes - 1) * around, 0)
    count = count + jnp.where(jnp.logical_and(head, group > 0), around - 1, 0)
    count = count + jnp.where(jnp.logical_and(head, group < n_groups - 1), 1, 0)

    @pl.when(jnp.logical_not(origin))
    def _():
        pl.semaphore_wait(barrier, count)

    entry, arrived, onward = 0, planes + 1, planes + 2
    entering = vector_ref.at[entry]

    @pl.when(origin)
    def _():
        vector_ref[arrived] = jnp.broadcast_to(window.first, (tail, state))

    for t in range(steps):
        kicks_ref[t, :, :state] = found[t]
    open_ref[...] = found[steps]
    offs_ref[0] = window.off_q
    offs_ref[1] = window.off_p
    rows_ref[0] = window.moved
    rows_ref[1] = window.landed
    plain = weights.hessians(window.curve_one, [curvature] * steps)
    for t in range(steps):
        kicks_ref[t, :, state:] = stationary(plain[t])

    to_lead = copy(run_ref, core_ref, core_sems.at[0], core_sems.at[1], place(inner_at=last))
    to_other = copy(pre_ref, pre_ref, pre_sems.at[0], pre_sems.at[1], place(inner_at=0))
    to_head = copy(
        majors_ref.at[plane], majors_ref.at[plane], majors_send, majors_recv.at[plane],
        place(group * planes),
    )

    def to_sub(t):
        return copy(
            subs_ref.at[sub], subs_ref.at[sub], subs_send.at[t], subs_recv.at[sub],
            place(sub_at=t),
        )

    @pl.when(jnp.logical_and(other, jnp.logical_not(origin)))
    def _():
        to_lead.start()

    @pl.when(lead)
    def _():
        @pl.when(opening_chip)
        def _():
            subs_ref[sub] = run_ref[...]

        @pl.when(jnp.logical_not(opening_chip))
        def _():
            to_lead.wait_recv()
            subs_ref[sub] = compose(core_ref[...], run_ref[...])

        for t in range(n_sub):
            @pl.when(gives_to(t))
            def _():
                to_sub(t).start()

        for s in range(n_sub):
            @pl.when(takes_from(s))
            def _():
                copy(
                    subs_ref.at[s], subs_ref.at[s], subs_send.at[s], subs_recv.at[s],
                    place(sub_at=s),
                ).wait_recv()

        pre_ref[...] = identity(state)
        for k in range(n_sub - 1):
            @pl.when(k < sub)
            def _():
                pre_ref[...] = compose(pre_ref[...], subs_ref[k])

        @pl.when(jnp.logical_not(opening_chip))
        def _():
            to_other.start()
            run_ref[...] = compose(pre_ref[...], core_ref[...])

        @pl.when(opening_chip)
        def _():
            run_ref[...] = identity(state)

        @pl.when(sub == 0)
        def _():
            majors_ref[plane] = chain([subs_ref[k] for k in range(n_sub)])

            @pl.when(plane > 0)
            def _():
                to_head.start()

            @pl.when(plane == 0)
            def _():
                ahead_ref[0] = majors_ref[0]
                for k in range(1, planes):
                    copy(
                        majors_ref.at[k], majors_ref.at[k], majors_send, majors_recv.at[k],
                        place(group * planes + k),
                    ).wait_recv()
                    ahead_ref[k] = compose(ahead_ref[k - 1], majors_ref[k])

    @pl.when(other)
    def _():
        @pl.when(origin)
        def _():
            run_ref[...] = identity(state)

        @pl.when(jnp.logical_not(origin))
        def _():
            to_lead.wait_send()
            to_other.wait_recv()
            run_ref[...] = pre_ref[...]

    coords, momenta = twice(run_ref[...])
    coords, momenta = with_tail(coords, -start_q), with_tail(momenta, -start_p)
    momenta = momenta - kick(coords, open_ref[...])

    def advance(t, carry):
        coords, momenta = carry
        coords = coords + step_size * momenta
        pair = kick(coords, kicks_ref[t])
        row = pl.ds(t, 1)
        maps_ref[t] = join(
            with_tail(coords, rows_ref[0, row, :]),
            with_tail(momenta - pair[:, state:], rows_ref[1, row, :]),
        )
        return (
            with_tail(coords, offs_ref[0, row, :]),
            with_tail(momenta - pair[:, :state], offs_ref[1, row, :]),
        )

    lax.fori_loop(0, steps - 1, advance, (coords, momenta))

    def to_next(source):
        return copy(source, entering, entry_send, entry_recv, place((group + 1) * planes))

    def to_each(act):
        def send(at, carry):
            @pl.when(at != last)
            def _():
                k = lax.div(at, around)
                act(copy(
                    vector_ref.at[k], vector_ref.at[arrived], spread_send.at[at], vector_recv,
                    place(
                        group * planes + k,
                        lax.rem(lax.div(at, n_inner), n_sub),
                        lax.rem(at, n_inner),
                    ),
                ))

            return carry

        lax.fori_loop(jnp.where(group > 0, 0, around), planes * around, send, 0)

    late = jnp.logical_and(tm == 0, jnp.logical_not(origin))

    @pl.when(late)
    def _():
        copy(guess_ref, raw_ref, spread_send.at[0], raw_recv, place(0, 0, 0)).wait_recv()
        left = jnp.broadcast_to(left_state(weights, raw_ref[...], start_ref[...]), (tail, state))
        vector_ref[entry] = left
        vector_ref[arrived] = left

    @pl.when(head)
    def _():
        @pl.when(group > 0)
        def _():
            to_next(vector_ref.at[onward]).wait_recv()

        here = vector_ref[entry, :1, :]
        for k in range(planes):
            slot = k + 1 if k + 1 < planes else onward
            vector_ref[slot] = jnp.broadcast_to(applied(here, ahead_ref[k]), (tail, state))

        @pl.when(group < n_groups - 1)
        def _():
            to_next(vector_ref.at[onward]).start()

        to_each(lambda c: c.start())
        vector_ref[arrived] = vector_ref[entry]

    @pl.when(jnp.logical_and(tm > 0, jnp.logical_not(head)))
    def _():
        copy(
            vector_ref.at[entry], vector_ref.at[arrived], spread_send.at[0], vector_recv,
            place(group * planes, 0, last),
        ).wait_recv()

    vector = vector_ref[arrived, :1, :]
    eye = iota((state, state), 0) == iota((state, state), 1)
    upright = jnp.sum(jnp.where(eye, vector, 0.0), axis=1, keepdims=True)
    for t in range(steps):
        ref = run_ref if t == 0 else maps_ref.at[t - 1]
        out_ref[t : t + 1, :] = (
            jnp.sum(upright * ref[:state, :], axis=0, keepdims=True) + ref[state : state + 1, :]
        )

    @pl.when(origin)
    def _():
        from_origin(lambda c: c.wait_send())

    @pl.when(lead)
    def _():
        for t in range(n_sub):
            @pl.when(gives_to(t))
            def _():
                to_sub(t).wait_send()

        @pl.when(jnp.logical_not(opening_chip))
        def _():
            to_other.wait_send()

        @pl.when(jnp.logical_and(column, plane > 0))
        def _():
            to_head.wait_send()

    @pl.when(head)
    def _():
        to_each(lambda c: c.wait_send())

        @pl.when(group < n_groups - 1)
        def _():
            to_next(vector_ref.at[onward]).wait_send()


def shards(sizes, guess, start, layer_weight, layer_bias, amplitude):
    n_tm, n_sub, n_inner = sizes
    steps, state = guess.shape
    rows = state + tail
    hidden = layer_bias.shape[0]
    vmem = pl.BlockSpec(memory_space=pltpu.VMEM)
    dma, regular = pltpu.SemaphoreType.DMA, pltpu.SemaphoreType.REGULAR
    return pl.pallas_call(
        functools.partial(kernel, sizes),
        out_shape=pltpu.VMEM((steps, state), f32),
        in_specs=[pl.BlockSpec(memory_space=pl.ANY)] * 5,
        out_specs=vmem,
        scratch_shapes=[
            pltpu.VMEM((steps, state), f32),
            pltpu.VMEM((1, state), f32),
            pltpu.VMEM((state // 2, hidden), f32),
            pltpu.VMEM((1, hidden), f32),
            pltpu.VMEM((1, hidden), f32),
            pltpu.VMEM((steps, 2 * state, 2 * state), bf16),
            pltpu.VMEM((2 * state, state), bf16),
            pltpu.VMEM((2, steps, state), f32),
            pltpu.VMEM((2, steps, state), f32),
            pltpu.VMEM((rows, state), f32),
            pltpu.VMEM((n_sub, rows, state), f32),
            pltpu.VMEM((planes, rows, state), f32),
            pltpu.VMEM((planes, rows, state), f32),
            pltpu.VMEM((rows, state), f32),
            pltpu.VMEM((rows, state), f32),
            pltpu.VMEM((3 + planes, tail, state), f32),
            pltpu.VMEM((steps, rows, state), f32),
            pltpu.VMEM((2 * state, hidden), bf16),
            pltpu.VMEM((hidden, 2 * state), bf16),
            pltpu.VMEM((steps, state), f32),
            dma((2,)),
            dma((n_sub,)),
            dma((n_sub,)),
            dma,
            dma((planes,)),
            dma((2,)),
            dma((planes * n_sub * n_inner,)),
            dma,
            dma,
            dma,
            dma,
            dma((5,)),
        ],
        compiler_params=pltpu.CompilerParams(collective_id=0, has_side_effects=True),
    )(guess, start.reshape(1, -1), layer_weight.T, layer_bias.reshape(1, -1), amplitude.reshape(1, -1))


def solution(mesh):
    sizes = tuple(mesh.shape[name] for name in ("tm", "sub", "inner"))
    placed = (P(("parts", "tm", "sub", "inner"), None), P("parts"), P(), P(), P())
    return jax.shard_map(
        functools.partial(shards, sizes),
        mesh=mesh,
        in_specs=placed,
        out_specs=P(("parts", "tm", "sub", "inner"), None),
        check_vma=False,
    )
```

```python
import functools

import jax
import jax.numpy as jnp
from jax import lax
from jax.experimental import pallas as pl
from jax.experimental.pallas import tpu as pltpu
from jax.sharding import PartitionSpec as P

step_size = 0.04
curvature = 0.5
half_step = 0.5 * step_size
f32, bf16 = jnp.float32, jnp.bfloat16
MESH = pl.DeviceIdType.MESH
planes = 4
tail = 8


def iota(shape, axis):
    return lax.broadcasted_iota(jnp.int32, shape, axis)


def split(value):
    high = value.astype(bf16)
    return high, (value - high.astype(f32)).astype(bf16)


def low_lanes(value):
    width = value.shape[-1]
    return iota(value.shape, 1) < width // 2


def mixed(value):
    high = value.astype(bf16).astype(f32)
    return jnp.where(low_lanes(value), high, value - high).astype(bf16)


def twice(value):
    swapped = pltpu.roll(value, value.shape[-1] // 2, 1)
    low = low_lanes(value)
    return jnp.where(low, value, swapped), jnp.where(low, swapped, value)


def join(coords, momenta):
    return jnp.where(low_lanes(coords), coords, momenta)


def dot(left, right):
    return jnp.dot(left, right, preferred_element_type=f32)


def with_tail(value, extra):
    rows = value.shape[0] - tail
    if rows == 0:
        return value + extra
    return jnp.concatenate([value[:rows], value[rows:] + extra], axis=0)


def compose(first, second):
    state = first.shape[1]
    eye = (iota((state, state), 0) == iota((state, state), 1)).astype(f32)
    high, low = split(second[:state] - eye)
    both = jnp.concatenate([high, low], axis=1)
    left = jnp.concatenate(split(first), axis=1)
    out = dot(left, jnp.concatenate([both, both], axis=0))
    return with_tail(first + (out[:, :state] + out[:, state:]), second[state:])


def chain(maps):
    while len(maps) > 1:
        maps = [
            compose(maps[k], maps[k + 1]) if k + 1 < len(maps) else maps[k]
            for k in range(0, len(maps), 2)
        ]
    return maps[0]


def identity(state):
    rows = state + tail
    return (iota((rows, state), 0) == iota((rows, state), 1)).astype(f32)


def diagonal_mask(state):
    return iota((state, state), 0) == iota((state, state), 1)


def stand(row):
    return jnp.sum(jnp.where(diagonal_mask(row.shape[1]), row, 0.0), axis=1, keepdims=True)


def laid(column, full):
    state = full.shape[1]
    return jnp.sum(column * full[:state], axis=0, keepdims=True) + full[state : state + 1]


def stood(row, full):
    state = full.shape[1]
    shift = jnp.where(diagonal_mask(state), full[state : state + 1], 0.0)
    return jnp.sum(full[:state].T * row + shift, axis=1, keepdims=True)


class Weights:
    def __init__(self, across_ref, onto_ref, back_ref, bias_ref, amplitude_ref):
        self.across_ref, self.onto_ref, self.back_ref = across_ref, onto_ref, back_ref
        self.bias_ref, self.amplitude_ref = bias_ref, amplitude_ref

    def fill(self, weight):
        across = jnp.concatenate([weight, weight], axis=0)
        high, low = split(across)
        self.onto_ref[...] = jnp.concatenate([high, low], axis=0)
        high, low = split(across.T)
        self.back_ref[...] = jnp.concatenate([high, low], axis=1)

    def along(self, value):
        left = mixed(value)
        return dot(jnp.concatenate([left, left], axis=1), self.onto_ref[...])

    def apart(self, value):
        back = self.back_ref[...]
        state = back.shape[1] // 2
        high, low = split(value)
        out = dot(high, back) + dot(low, back)
        return out[:, :state] + out[:, state:]

    def forces(self, coords):
        gate = 1.0 / (1.0 + jnp.exp(-(self.along(coords) + self.bias_ref[...])))
        pull = self.amplitude_ref[...] * gate
        return self.apart(pull) + curvature * coords, pull * (1.0 - gate)

    def hessians(self, curves, diagonal):
        count = curves.shape[0]
        across, back = self.across_ref[...], self.back_ref[...]
        width, state = across.shape[0], back.shape[1] // 2
        parts = [split(across * curves[k : k + 1]) for k in range(count)]
        stacked = jnp.concatenate([p[0] for p in parts] + [p[1] for p in parts], axis=0)
        out = dot(stacked, back)
        out = out[:, :state] + out[:, state:]
        out = out[: count * width] + out[count * width :]
        unit = jnp.where(iota((width, state), 0) == iota((width, state), 1) % width, 1.0, 0.0)
        return [out[k * width : (k + 1) * width] + diagonal[k] * unit for k in range(count)]


def stationary(hessian):
    high, low = split(hessian)
    return jnp.concatenate([high, high, low, low], axis=0)


class Window:
    def __init__(self, weights, rows, start):
        self.steps, self.state = steps, state = rows.shape
        coords, momenta = twice(
            jnp.concatenate([rows, jnp.broadcast_to(start, (tail, state))], axis=0)
        )
        grad_zero, curve_zero = weights.forces(coords)
        half = momenta - half_step * grad_zero
        moved = coords + step_size * half
        grad_one, curve_one = weights.forces(moved)
        landed = half - half_step * grad_one
        self.first_q, self.first_p = moved[steps:], landed[steps:]
        self.first = join(self.first_q, self.first_p)[:1]
        coords, momenta = coords[:steps], momenta[:steps]
        self.curve_zero, self.curve_one = curve_zero[:steps], curve_one[:steps]
        self.moved, self.landed = moved[:steps], landed[:steps]
        self.start_q, self.start_p = coords[:1], momenta[:1]
        inside = iota((steps, 1), 0) < steps - 1

        def later(value):
            return jnp.where(inside, pltpu.roll(value, steps - 1, 0), 0.0)

        curve_next = later(self.curve_zero)
        opening = jnp.broadcast_to(self.curve_zero[:1], (tail, self.curve_zero.shape[1]))
        self.curves = jnp.concatenate([self.curve_one + curve_next, opening], axis=0)[: steps + 1]
        self.diagonal = [2.0 * curvature] * (steps - 1) + [curvature, curvature]
        self.off_q = self.moved - later(coords)
        begin_q = self.first_q - self.start_q
        begin_p = self.first_p - self.start_p
        pulled = jnp.concatenate([jnp.where(inside, self.off_q, 0.0), begin_q], axis=0)
        curve = jnp.concatenate([curve_next, opening], axis=0)
        kicked = half_step * (weights.apart(weights.along(pulled) * curve) + curvature * pulled)
        self.off_p = self.landed - later(momenta) - kicked[:steps]
        self.begin_q, self.begin_p = begin_q, begin_p - kicked[steps:]


def kick(coords, kicks):
    left = mixed(coords)
    return half_step * dot(jnp.concatenate([left, left], axis=1), kicks)


def window_map(window, kicks):
    steps, state = window.steps, window.state
    runs = 4
    length = steps // runs
    ident = identity(state)
    states = []
    for c in range(runs):
        coords, momenta = twice(ident)
        if c == 0:
            coords = with_tail(coords, -window.start_q)
            momenta = with_tail(momenta, -window.start_p)
            momenta = momenta - kick(coords, kicks[steps])
        states.append((coords, momenta))
    for j in range(length):
        for c in range(runs):
            t = c * length + j
            coords, momenta = states[c]
            coords = coords + step_size * momenta
            momenta = momenta - kick(coords, kicks[t])
            states[c] = (
                with_tail(coords, window.off_q[t : t + 1]),
                with_tail(momenta, window.off_p[t : t + 1]),
            )
    return chain([join(*s) for s in states])


def run_lengths(steps):
    return [steps // 4] * 4


def left_state(weights, rows, start):
    window = Window(weights, rows, start)
    steps, state = window.steps, window.state
    width = state // 2
    lengths = run_lengths(steps)
    begins = [sum(lengths[:c]) for c in range(len(lengths))]
    hessians = weights.hessians(window.curves[:steps], window.diagonal)
    repeated = jnp.where(iota((width, state), 0) == iota((width, state), 1) % width, 1.0, 0.0)
    none = jnp.zeros((tail, state), f32)
    moving = jnp.concatenate([repeated, step_size * repeated, none], axis=0)
    states = [(window.begin_q, window.begin_p)]
    for t in begins[1:]:
        bend = half_step * hessians[t]
        momenta = jnp.concatenate([-bend, repeated - step_size * bend, none], axis=0)
        states.append((
            with_tail(moving, window.off_q[t : t + 1]),
            with_tail(momenta, window.off_p[t : t + 1]),
        ))
    for j in range(max(lengths)):
        for c, length in enumerate(lengths):
            t = begins[c] + j + (1 if c else 0)
            if t >= begins[c] + length:
                continue
            coords, momenta = states[c]
            coords = coords + step_size * momenta
            momenta = momenta - kick(coords, stationary(hessians[t]))
            states[c] = (
                with_tail(coords, window.off_q[t : t + 1]),
                with_tail(momenta, window.off_p[t : t + 1]),
            )
    maps = [join(*s) for s in states]
    vector, upright = maps[0][:1], False
    for full in maps[1:]:
        vector = laid(vector, full) if upright else stood(vector, full)
        upright = not upright
    return vector if upright else stand(vector)


def kernel(
    sizes, guess_hbm, start_hbm, weight_hbm, bias_hbm, amplitude_hbm, out_ref,
    guess_ref, start_ref, weight_ref, bias_ref, amplitude_ref,
    kicks_ref, open_ref, offs_ref, rows_ref, core_ref, subs_ref, majors_ref, ahead_ref,
    pre_ref, run_ref, vector_ref, maps_ref, onto_ref, back_ref, raw_ref,
    upright_ref, pair_send, pair_recv, subs_send, subs_recv, column_send, majors_recv,
    spread_send, state_recv, load_guess, load_last,
):
    n_tm, n_sub, n_inner = sizes
    n_groups = n_tm // planes
    part, tm = lax.axis_index("parts"), lax.axis_index("tm")
    sub, inner = lax.axis_index("sub"), lax.axis_index("inner")
    group, plane = lax.div(tm, planes), lax.rem(tm, planes)
    steps, state = guess_ref.shape
    last = n_inner - 1
    lead = inner == last
    other = jnp.logical_not(lead)
    column = jnp.logical_and(lead, sub == 0)
    head = jnp.logical_and(column, plane == 0)
    opening_chip = jnp.logical_and(tm == 0, sub == 0)
    origin = jnp.logical_and(opening_chip, inner == 0)

    def place(tm_at=None, sub_at=None, inner_at=None):
        return (
            part,
            tm if tm_at is None else tm_at,
            sub if sub_at is None else sub_at,
            inner if inner_at is None else inner_at,
        )

    def copy(source, target, send, recv, where):
        return pltpu.make_async_remote_copy(
            src_ref=source, dst_ref=target, send_sem=send, recv_sem=recv,
            device_id=where, device_id_type=MESH,
        )

    def both(*conditions):
        return functools.reduce(jnp.logical_and, conditions)

    barrier = pltpu.get_barrier_semaphore()
    around = n_sub * n_inner
    loads = [
        pltpu.make_async_copy(source, target, sem)
        for source, target, sem in (
            (guess_hbm, guess_ref, load_guess), (weight_hbm, weight_ref, subs_send),
            (start_hbm, start_ref, column_send), (bias_hbm, bias_ref, pair_send),
            (amplitude_hbm, amplitude_ref, load_last),
        )
    ]
    loads[0].start()

    def from_origin(at):
        return copy(
            guess_ref, raw_ref, spread_send, state_recv, place(0, at // n_inner, at % n_inner)
        )

    @pl.when(origin)
    def _():
        pl.semaphore_wait(barrier, around - 1)
        loads[0].wait()
        for at in range(1, around):
            from_origin(at).start()

    for load in loads[1:]:
        load.start()

    @pl.when(jnp.logical_not(origin))
    def _():
        loads[0].wait()

    def greet(where):
        pl.semaphore_signal(barrier, inc=1, device_id=where, device_id_type=MESH)

    @pl.when(jnp.logical_not(origin))
    def _():
        @pl.when(jnp.logical_not(both(opening_chip, lead)))
        def _():
            greet(place(inner_at=n_inner - 1 - inner))

        @pl.when(tm == 0)
        def _():
            greet(place(0, 0, 0))

        @pl.when(both(tm > 0, jnp.logical_not(column)))
        def _():
            greet(place(tm, 0, last))

        @pl.when(both(column, plane > 0))
        def _():
            greet(place(group * planes))

    def takes_from(s):
        return both(lead, sub != s, jnp.logical_or(sub > s, sub == 0))

    def gives_to(t):
        return both(lead, sub != t, jnp.logical_or(sub < t, t == 0))

    for s in range(n_sub):
        @pl.when(takes_from(s))
        def _():
            greet(place(sub_at=s))

    @pl.when(head)
    def _():
        for k in range(1, planes):
            greet(place(group * planes + k))

        @pl.when(group > 0)
        def _():
            greet(place((group - 1) * planes))

    for load in loads[1:]:
        load.wait()
    weights = Weights(weight_ref, onto_ref, back_ref, bias_ref, amplitude_ref)
    weights.fill(weight_ref[...])
    start = start_ref[...]
    window = Window(weights, guess_ref[...], start)
    found = [stationary(k) for k in weights.hessians(window.curves, window.diagonal)]
    run_ref[...] = window_map(window, found)
    start_q, start_p = window.start_q, window.start_p

    count = jnp.where(jnp.logical_and(lead, jnp.logical_not(opening_chip)), 1, 0)
    count = count + jnp.where(other, 1, 0)
    count = count + jnp.where(lead, jnp.where(sub == 0, n_sub - 1, n_sub - sub), 0)
    count = count + jnp.where(jnp.logical_and(column, plane > 0), 1, 0)
    count = count + jnp.where(head, planes - 1, 0)
    count = count + jnp.where(jnp.logical_and(column, tm > 0), around - 1, 0)
    count = count + jnp.where(jnp.logical_and(head, group < n_groups - 1), 1, 0)

    @pl.when(jnp.logical_not(origin))
    def _():
        pl.semaphore_wait(barrier, count)

    entry, arrived, onward = 0, planes + 1, planes + 2

    @pl.when(origin)
    def _():
        upright_ref[...] = jnp.broadcast_to(stand(window.first), (state, state))

    for t in range(steps):
        kicks_ref[t, :, :state] = found[t]
    open_ref[...] = found[steps]
    offs_ref[0] = window.off_q
    offs_ref[1] = window.off_p
    rows_ref[0] = window.moved
    rows_ref[1] = window.landed
    plain = weights.hessians(window.curve_one, [curvature] * steps)
    for t in range(steps):
        kicks_ref[t, :, state:] = stationary(plain[t])

    to_lead = copy(run_ref, core_ref, pair_send, pair_recv, place(inner_at=last))
    to_other = copy(pre_ref, pre_ref, pair_send, pair_recv, place(inner_at=0))
    to_head = copy(
        majors_ref.at[plane], majors_ref.at[plane], column_send, majors_recv,
        place(group * planes),
    )

    def to_sub(t):
        return copy(
            subs_ref.at[sub], subs_ref.at[sub], subs_send, subs_recv, place(sub_at=t)
        )

    def some_subs(count):
        part_of = subs_ref.at[pl.ds(0, count)]
        return copy(part_of, part_of, subs_send, subs_recv, place())

    given = jnp.where(sub == 0, n_sub - 1, n_sub - sub)
    taken = jnp.where(sub == 0, n_sub - 1, sub)

    @pl.when(jnp.logical_and(other, jnp.logical_not(origin)))
    def _():
        to_lead.start()

    @pl.when(lead)
    def _():
        @pl.when(opening_chip)
        def _():
            subs_ref[sub] = run_ref[...]

        @pl.when(jnp.logical_not(opening_chip))
        def _():
            to_lead.wait_recv()
            subs_ref[sub] = compose(core_ref[...], run_ref[...])

        for t in range(n_sub):
            @pl.when(gives_to(t))
            def _():
                to_sub(t).start()

        for k in range(1, n_sub):
            @pl.when(taken == k)
            def _():
                some_subs(k).wait_recv()

        pre_ref[...] = identity(state)
        for k in range(n_sub - 1):
            @pl.when(k < sub)
            def _():
                pre_ref[...] = compose(pre_ref[...], subs_ref[k])

        @pl.when(jnp.logical_not(opening_chip))
        def _():
            to_other.start()
            run_ref[...] = compose(pre_ref[...], core_ref[...])

        @pl.when(opening_chip)
        def _():
            run_ref[...] = identity(state)

        @pl.when(sub == 0)
        def _():
            majors_ref[plane] = chain([subs_ref[k] for k in range(n_sub)])

            @pl.when(plane > 0)
            def _():
                to_head.start()

            @pl.when(plane == 0)
            def _():
                ahead_ref[0] = majors_ref[0]
                others = majors_ref.at[pl.ds(1, planes - 1)]
                copy(others, others, column_send, majors_recv, place()).wait_recv()
                for k in range(1, planes):
                    ahead_ref[k] = compose(ahead_ref[k - 1], majors_ref[k])

    @pl.when(other)
    def _():
        @pl.when(origin)
        def _():
            run_ref[...] = identity(state)

        @pl.when(jnp.logical_not(origin))
        def _():
            to_lead.wait_send()
            to_other.wait_recv()
            run_ref[...] = pre_ref[...]

    coords, momenta = twice(run_ref[...])
    coords, momenta = with_tail(coords, -start_q), with_tail(momenta, -start_p)
    momenta = momenta - kick(coords, open_ref[...])

    def advance(t, carry):
        coords, momenta = carry
        coords = coords + step_size * momenta
        pair = kick(coords, kicks_ref[t])
        row = pl.ds(t, 1)
        maps_ref[t] = join(
            with_tail(coords, rows_ref[0, row, :]),
            with_tail(momenta - pair[:, state:], rows_ref[1, row, :]),
        )
        return (
            with_tail(coords, offs_ref[0, row, :]),
            with_tail(momenta - pair[:, :state], offs_ref[1, row, :]),
        )

    lax.fori_loop(0, steps - 1, advance, (coords, momenta))

    to_next = copy(
        vector_ref.at[onward], vector_ref.at[entry], column_send, state_recv,
        place((group + 1) * planes),
    )

    def to_plane(k):
        return copy(
            vector_ref.at[k], vector_ref.at[arrived], spread_send, state_recv,
            place(group * planes + k),
        )

    def to_device(at):
        return copy(
            vector_ref.at[arrived], vector_ref.at[arrived], spread_send, state_recv,
            place(tm, at // n_inner, at % n_inner),
        )

    def spread():
        for at in range(around):
            if at != last:
                to_device(at).start()

    def stand_at(slot):
        upright_ref[...] = jnp.broadcast_to(stand(vector_ref[slot]), (state, state))

    @pl.when(jnp.logical_and(tm == 0, jnp.logical_not(origin)))
    def _():
        copy(guess_ref, raw_ref, spread_send, state_recv, place(0, 0, 0)).wait_recv()
        left = left_state(weights, raw_ref[...], start_ref[...])
        upright_ref[...] = jnp.broadcast_to(left, (state, state))

    @pl.when(head)
    def _():
        @pl.when(group > 0)
        def _():
            to_next.wait_recv()
            stand_at(entry)

        for k in range(planes):
            vector_ref[k + 1 if k + 1 < planes else onward] = laid(upright_ref[...], ahead_ref[k])

        @pl.when(group < n_groups - 1)
        def _():
            to_next.start()

        for k in range(1, planes):
            to_plane(k).start()

        @pl.when(group > 0)
        def _():
            vector_ref[arrived] = vector_ref[entry]
            spread()

    @pl.when(jnp.logical_and(tm > 0, jnp.logical_not(head)))
    def _():
        to_device(0).wait_recv()

        @pl.when(column)
        def _():
            spread()

        stand_at(arrived)

    upright = upright_ref[...]
    for t in range(steps):
        ref = run_ref if t == 0 else maps_ref.at[t - 1]
        out_ref[t : t + 1, :] = laid(upright, ref)

    def spread_left(rows):
        sent = maps_ref.at[0, pl.ds(0, rows), :]
        copy(sent, sent, spread_send, state_recv, place()).wait_send()

    @pl.when(origin)
    def _():
        spread_left((around - 1) * steps)

    @pl.when(lead)
    def _():
        for k in range(1, n_sub):
            @pl.when(given == k)
            def _():
                some_subs(k).wait_send()

        @pl.when(jnp.logical_not(opening_chip))
        def _():
            to_other.wait_send()

        @pl.when(jnp.logical_and(column, plane > 0))
        def _():
            to_head.wait_send()

    @pl.when(column)
    def _():
        ahead = planes - 1

        @pl.when(both(head, tm > 0))
        def _():
            spread_left(ahead + around - 1)

        @pl.when(both(head, tm == 0))
        def _():
            spread_left(ahead)

        @pl.when(plane > 0)
        def _():
            spread_left(around - 1)

    @pl.when(both(head, group < n_groups - 1))
    def _():
        to_next.wait_send()


def shards(sizes, guess, start, layer_weight, layer_bias, amplitude):
    n_tm, n_sub, n_inner = sizes
    steps, state = guess.shape
    rows = state + tail
    hidden = layer_bias.shape[0]
    vmem = pl.BlockSpec(memory_space=pltpu.VMEM)
    dma = pltpu.SemaphoreType.DMA
    return pl.pallas_call(
        functools.partial(kernel, sizes),
        out_shape=pltpu.VMEM((steps, state), f32),
        in_specs=[pl.BlockSpec(memory_space=pl.ANY)] * 5,
        out_specs=vmem,
        scratch_shapes=[
            pltpu.VMEM((steps, state), f32),
            pltpu.VMEM((1, state), f32),
            pltpu.VMEM((state // 2, hidden), f32),
            pltpu.VMEM((1, hidden), f32),
            pltpu.VMEM((1, hidden), f32),
            pltpu.VMEM((steps, 2 * state, 2 * state), bf16),
            pltpu.VMEM((2 * state, state), bf16),
            pltpu.VMEM((2, steps, state), f32),
            pltpu.VMEM((2, steps, state), f32),
            pltpu.VMEM((rows, state), f32),
            pltpu.VMEM((n_sub, rows, state), f32),
            pltpu.VMEM((planes, rows, state), f32),
            pltpu.VMEM((planes, rows, state), f32),
            pltpu.VMEM((rows, state), f32),
            pltpu.VMEM((rows, state), f32),
            pltpu.VMEM((3 + planes, 1, state), f32),
            pltpu.VMEM((steps, rows, state), f32),
            pltpu.VMEM((2 * state, hidden), bf16),
            pltpu.VMEM((hidden, 2 * state), bf16),
            pltpu.VMEM((steps, state), f32),
            pltpu.VMEM((state, state), f32),
            dma,
            dma,
            dma,
            dma,
            dma,
            dma,
            dma,
            dma,
            dma,
            dma,
        ],
        compiler_params=pltpu.CompilerParams(collective_id=0, has_side_effects=True),
    )(guess, start.reshape(1, -1), layer_weight.T, layer_bias.reshape(1, -1), amplitude.reshape(1, -1))


def solution(mesh):
    sizes = tuple(mesh.shape[name] for name in ("tm", "sub", "inner"))
    placed = (P(("parts", "tm", "sub", "inner"), None), P("parts"), P(), P(), P())
    return jax.shard_map(
        functools.partial(shards, sizes),
        mesh=mesh,
        in_specs=placed,
        out_specs=P(("parts", "tm", "sub", "inner"), None),
        check_vma=False,
    )
```

```python
import functools

import jax
import jax.numpy as jnp
from jax import lax
from jax.experimental import pallas as pl
from jax.experimental.pallas import tpu as pltpu
from jax.sharding import PartitionSpec as P

step_size = 0.04
curvature = 0.5
half_step = 0.5 * step_size
f32, bf16 = jnp.float32, jnp.bfloat16
MESH = pl.DeviceIdType.MESH
planes = 4
home = 1
tail = 8


def iota(shape, axis):
    return lax.broadcasted_iota(jnp.int32, shape, axis)


def split(value):
    high = value.astype(bf16)
    return high, (value - high.astype(f32)).astype(bf16)


def low_lanes(value):
    width = value.shape[-1]
    return iota(value.shape, 1) < width // 2


def mixed(value):
    high = value.astype(bf16).astype(f32)
    return jnp.where(low_lanes(value), high, value - high).astype(bf16)


def twice(value):
    swapped = pltpu.roll(value, value.shape[-1] // 2, 1)
    low = low_lanes(value)
    return jnp.where(low, value, swapped), jnp.where(low, swapped, value)


def join(coords, momenta):
    return jnp.where(low_lanes(coords), coords, momenta)


def dot(left, right):
    return jnp.dot(left, right, preferred_element_type=f32)


def with_tail(value, extra):
    rows = value.shape[0] - tail
    if rows == 0:
        return value + extra
    return jnp.concatenate([value[:rows], value[rows:] + extra], axis=0)


def compose(first, second):
    state = first.shape[1]
    eye = (iota((state, state), 0) == iota((state, state), 1)).astype(f32)
    high, low = split(second[:state] - eye)
    both = jnp.concatenate([high, low], axis=1)
    left = jnp.concatenate(split(first), axis=1)
    out = dot(left, jnp.concatenate([both, both], axis=0))
    return with_tail(first + (out[:, :state] + out[:, state:]), second[state:])


def chain(maps):
    while len(maps) > 1:
        maps = [
            compose(maps[k], maps[k + 1]) if k + 1 < len(maps) else maps[k]
            for k in range(0, len(maps), 2)
        ]
    return maps[0]


def identity(state):
    rows = state + tail
    return (iota((rows, state), 0) == iota((rows, state), 1)).astype(f32)


def diagonal_mask(state):
    return iota((state, state), 0) == iota((state, state), 1)


def stand(row):
    return jnp.sum(jnp.where(diagonal_mask(row.shape[1]), row, 0.0), axis=1, keepdims=True)


def laid(column, full):
    state = full.shape[1]
    return jnp.sum(column * full[:state], axis=0, keepdims=True) + full[state : state + 1]


def stood(row, full):
    state = full.shape[1]
    shift = jnp.where(diagonal_mask(state), full[state : state + 1], 0.0)
    return jnp.sum(full[:state].T * row + shift, axis=1, keepdims=True)


class Weights:
    def __init__(self, across_ref, onto_ref, back_ref, bias_ref, amplitude_ref):
        self.across_ref, self.onto_ref, self.back_ref = across_ref, onto_ref, back_ref
        self.bias_ref, self.amplitude_ref = bias_ref, amplitude_ref

    def fill(self, weight):
        across = jnp.concatenate([weight, weight], axis=0)
        high, low = split(across)
        self.onto_ref[...] = jnp.concatenate([high, low], axis=0)
        high, low = split(across.T)
        self.back_ref[...] = jnp.concatenate([high, low], axis=1)

    def along(self, value):
        left = mixed(value)
        return dot(jnp.concatenate([left, left], axis=1), self.onto_ref[...])

    def apart(self, value):
        back = self.back_ref[...]
        state = back.shape[1] // 2
        high, low = split(value)
        out = dot(high, back) + dot(low, back)
        return out[:, :state] + out[:, state:]

    def forces(self, coords):
        gate = 1.0 / (1.0 + jnp.exp(-(self.along(coords) + self.bias_ref[...])))
        pull = self.amplitude_ref[...] * gate
        return self.apart(pull) + curvature * coords, pull * (1.0 - gate)

    def hessians(self, curves, diagonal):
        count = curves.shape[0]
        across, back = self.across_ref[...], self.back_ref[...]
        width, state = across.shape[0], back.shape[1] // 2
        parts = [split(across * curves[k : k + 1]) for k in range(count)]
        stacked = jnp.concatenate([p[0] for p in parts] + [p[1] for p in parts], axis=0)
        out = dot(stacked, back)
        out = out[:, :state] + out[:, state:]
        out = out[: count * width] + out[count * width :]
        unit = jnp.where(iota((width, state), 0) == iota((width, state), 1) % width, 1.0, 0.0)
        return [out[k * width : (k + 1) * width] + diagonal[k] * unit for k in range(count)]


def stationary(hessian):
    high, low = split(hessian)
    return jnp.concatenate([high, high, low, low], axis=0)


class Window:
    def __init__(self, weights, rows, start):
        self.steps, self.state = steps, state = rows.shape
        coords, momenta = twice(
            jnp.concatenate([rows, jnp.broadcast_to(start, (tail, state))], axis=0)
        )
        grad_zero, curve_zero = weights.forces(coords)
        half = momenta - half_step * grad_zero
        moved = coords + step_size * half
        grad_one, curve_one = weights.forces(moved)
        landed = half - half_step * grad_one
        self.first_q, self.first_p = moved[steps:], landed[steps:]
        self.first = join(self.first_q, self.first_p)[:1]
        coords, momenta = coords[:steps], momenta[:steps]
        self.curve_zero, self.curve_one = curve_zero[:steps], curve_one[:steps]
        self.moved, self.landed = moved[:steps], landed[:steps]
        self.start_q, self.start_p = coords[:1], momenta[:1]
        inside = iota((steps, 1), 0) < steps - 1

        def later(value):
            return jnp.where(inside, pltpu.roll(value, steps - 1, 0), 0.0)

        curve_next = later(self.curve_zero)
        opening = jnp.broadcast_to(self.curve_zero[:1], (tail, self.curve_zero.shape[1]))
        self.curves = jnp.concatenate([self.curve_one + curve_next, opening], axis=0)[: steps + 1]
        self.diagonal = [2.0 * curvature] * (steps - 1) + [curvature, curvature]
        self.off_q = self.moved - later(coords)
        begin_q = self.first_q - self.start_q
        begin_p = self.first_p - self.start_p
        pulled = jnp.concatenate([jnp.where(inside, self.off_q, 0.0), begin_q], axis=0)
        curve = jnp.concatenate([curve_next, opening], axis=0)
        kicked = half_step * (weights.apart(weights.along(pulled) * curve) + curvature * pulled)
        self.off_p = self.landed - later(momenta) - kicked[:steps]
        self.begin_q, self.begin_p = begin_q, begin_p - kicked[steps:]


def kick(coords, kicks):
    left = mixed(coords)
    return half_step * dot(jnp.concatenate([left, left], axis=1), kicks)


def window_map(window, kicks):
    steps, state = window.steps, window.state
    runs = 4
    length = steps // runs
    ident = identity(state)
    states = []
    for c in range(runs):
        coords, momenta = twice(ident)
        if c == 0:
            coords = with_tail(coords, -window.start_q)
            momenta = with_tail(momenta, -window.start_p)
            momenta = momenta - kick(coords, kicks[steps])
        states.append((coords, momenta))
    for j in range(length):
        for c in range(runs):
            t = c * length + j
            coords, momenta = states[c]
            coords = coords + step_size * momenta
            momenta = momenta - kick(coords, kicks[t])
            states[c] = (
                with_tail(coords, window.off_q[t : t + 1]),
                with_tail(momenta, window.off_p[t : t + 1]),
            )
    return chain([join(*s) for s in states])


def run_lengths(steps):
    return [steps // 4] * 4


def left_state(weights, rows, start):
    window = Window(weights, rows, start)
    steps, state = window.steps, window.state
    width = state // 2
    lengths = run_lengths(steps)
    begins = [sum(lengths[:c]) for c in range(len(lengths))]
    hessians = weights.hessians(window.curves[:steps], window.diagonal)
    repeated = jnp.where(iota((width, state), 0) == iota((width, state), 1) % width, 1.0, 0.0)
    none = jnp.zeros((tail, state), f32)
    moving = jnp.concatenate([repeated, step_size * repeated, none], axis=0)
    states = [(window.begin_q, window.begin_p)]
    for t in begins[1:]:
        bend = half_step * hessians[t]
        momenta = jnp.concatenate([-bend, repeated - step_size * bend, none], axis=0)
        states.append((
            with_tail(moving, window.off_q[t : t + 1]),
            with_tail(momenta, window.off_p[t : t + 1]),
        ))
    for j in range(max(lengths)):
        for c, length in enumerate(lengths):
            t = begins[c] + j + (1 if c else 0)
            if t >= begins[c] + length:
                continue
            coords, momenta = states[c]
            coords = coords + step_size * momenta
            momenta = momenta - kick(coords, stationary(hessians[t]))
            states[c] = (
                with_tail(coords, window.off_q[t : t + 1]),
                with_tail(momenta, window.off_p[t : t + 1]),
            )
    maps = [join(*s) for s in states]
    vector, upright = maps[0][:1], False
    for full in maps[1:]:
        vector = laid(vector, full) if upright else stood(vector, full)
        upright = not upright
    return vector if upright else stand(vector)


def kernel(
    sizes, guess_hbm, start_hbm, weight_hbm, bias_hbm, amplitude_hbm, out_ref,
    guess_ref, start_ref, weight_ref, bias_ref, amplitude_ref,
    kicks_ref, open_ref, offs_ref, rows_ref, core_ref, subs_ref, majors_ref, ahead_ref,
    pre_ref, run_ref, vector_ref, maps_ref, onto_ref, back_ref, raw_ref,
    upright_ref, pair_send, pair_recv, subs_send, subs_recv, column_send, majors_recv,
    spread_send, state_recv, load_guess, load_last,
):
    n_tm, n_sub, n_inner = sizes
    n_groups = n_tm // planes
    part, tm = lax.axis_index("parts"), lax.axis_index("tm")
    sub, inner = lax.axis_index("sub"), lax.axis_index("inner")
    group, plane = lax.div(tm, planes), lax.rem(tm, planes)
    steps, state = guess_ref.shape
    last = n_inner - 1
    lead = inner == last
    other = jnp.logical_not(lead)
    column = jnp.logical_and(lead, sub == 0)
    head = jnp.logical_and(column, plane == home)
    opening_chip = jnp.logical_and(tm == 0, sub == 0)
    origin = jnp.logical_and(opening_chip, inner == 0)
    starts = jnp.logical_and(
        jnp.logical_not(origin), jnp.logical_or(tm == 0, jnp.logical_and(head, group == 0))
    )

    def place(tm_at=None, sub_at=None, inner_at=None):
        return (
            part,
            tm if tm_at is None else tm_at,
            sub if sub_at is None else sub_at,
            inner if inner_at is None else inner_at,
        )

    def copy(source, target, send, recv, where):
        return pltpu.make_async_remote_copy(
            src_ref=source, dst_ref=target, send_sem=send, recv_sem=recv,
            device_id=where, device_id_type=MESH,
        )

    def both(*conditions):
        return functools.reduce(jnp.logical_and, conditions)

    barrier = pltpu.get_barrier_semaphore()
    around = n_sub * n_inner
    loads = [
        pltpu.make_async_copy(source, target, sem)
        for source, target, sem in (
            (guess_hbm, guess_ref, load_guess), (weight_hbm, weight_ref, subs_send),
            (start_hbm, start_ref, column_send), (bias_hbm, bias_ref, pair_send),
            (amplitude_hbm, amplitude_ref, load_last),
        )
    ]
    loads[0].start()

    def from_origin(at):
        where = place(0, at // n_inner, at % n_inner) if at < around else place(home, 0, last)
        return copy(guess_ref, raw_ref, spread_send, state_recv, where)

    @pl.when(origin)
    def _():
        pl.semaphore_wait(barrier, around)
        loads[0].wait()
        for at in range(1, around + 1):
            from_origin(at).start()

    for load in loads[1:]:
        load.start()

    @pl.when(jnp.logical_not(origin))
    def _():
        loads[0].wait()

    def greet(where):
        pl.semaphore_signal(barrier, inc=1, device_id=where, device_id_type=MESH)

    @pl.when(jnp.logical_not(origin))
    def _():
        @pl.when(jnp.logical_not(both(opening_chip, lead)))
        def _():
            greet(place(inner_at=n_inner - 1 - inner))

        @pl.when(starts)
        def _():
            greet(place(0, 0, 0))

        @pl.when(both(tm > 0, jnp.logical_not(column)))
        def _():
            greet(place(tm, 0, last))

        @pl.when(both(column, tm > 0, plane != home))
        def _():
            greet(place(group * planes + home))

    def takes_from(s):
        return both(lead, sub != s, jnp.logical_or(sub > s, sub == 0))

    def gives_to(t):
        return both(lead, sub != t, jnp.logical_or(sub < t, t == 0))

    for s in range(n_sub):
        @pl.when(takes_from(s))
        def _():
            greet(place(sub_at=s))

    @pl.when(head)
    def _():
        for k in range(planes):
            if k != home:
                greet(place(group * planes + k))

        @pl.when(group > 0)
        def _():
            greet(place((group - 1) * planes + home))

    for load in loads[1:]:
        load.wait()
    weights = Weights(weight_ref, onto_ref, back_ref, bias_ref, amplitude_ref)
    weights.fill(weight_ref[...])
    start = start_ref[...]
    window = Window(weights, guess_ref[...], start)
    found = [stationary(k) for k in weights.hessians(window.curves, window.diagonal)]
    run_ref[...] = window_map(window, found)
    start_q, start_p = window.start_q, window.start_p

    count = jnp.where(jnp.logical_and(lead, jnp.logical_not(opening_chip)), 1, 0)
    count = count + jnp.where(other, 1, 0)
    count = count + jnp.where(lead, jnp.where(sub == 0, n_sub - 1, n_sub - sub), 0)
    count = count + jnp.where(jnp.logical_and(column, plane != home), 1, 0)
    count = count + jnp.where(head, jnp.where(group > 0, planes - 1, planes - 2), 0)
    count = count + jnp.where(jnp.logical_and(column, tm > 0), around - 1, 0)
    count = count + jnp.where(jnp.logical_and(head, group < n_groups - 1), 1, 0)

    @pl.when(jnp.logical_not(origin))
    def _():
        pl.semaphore_wait(barrier, count)

    entry, arrived, onward = 0, planes + 1, planes + 2

    @pl.when(origin)
    def _():
        upright_ref[...] = jnp.broadcast_to(stand(window.first), (state, state))

    for t in range(steps):
        kicks_ref[t, :, :state] = found[t]
    open_ref[...] = found[steps]
    offs_ref[0] = window.off_q
    offs_ref[1] = window.off_p
    rows_ref[0] = window.moved
    rows_ref[1] = window.landed
    plain = weights.hessians(window.curve_one, [curvature] * steps)
    for t in range(steps):
        kicks_ref[t, :, state:] = stationary(plain[t])

    to_lead = copy(run_ref, core_ref, pair_send, pair_recv, place(inner_at=last))
    to_other = copy(pre_ref, pre_ref, pair_send, pair_recv, place(inner_at=0))
    to_head = copy(
        majors_ref.at[plane], majors_ref.at[plane], column_send, majors_recv,
        place(group * planes + home),
    )

    def to_sub(t):
        return copy(
            subs_ref.at[sub], subs_ref.at[sub], subs_send, subs_recv, place(sub_at=t)
        )

    def some_subs(count):
        part_of = subs_ref.at[pl.ds(0, count)]
        return copy(part_of, part_of, subs_send, subs_recv, place())

    given = jnp.where(sub == 0, n_sub - 1, n_sub - sub)
    taken = jnp.where(sub == 0, n_sub - 1, sub)

    @pl.when(jnp.logical_and(other, jnp.logical_not(origin)))
    def _():
        to_lead.start()

    @pl.when(lead)
    def _():
        @pl.when(opening_chip)
        def _():
            subs_ref[sub] = run_ref[...]

        @pl.when(jnp.logical_not(opening_chip))
        def _():
            to_lead.wait_recv()
            subs_ref[sub] = compose(core_ref[...], run_ref[...])

        for t in range(n_sub):
            @pl.when(gives_to(t))
            def _():
                to_sub(t).start()

        for k in range(1, n_sub):
            @pl.when(taken == k)
            def _():
                some_subs(k).wait_recv()

        pre_ref[...] = identity(state)
        for k in range(n_sub - 1):
            @pl.when(k < sub)
            def _():
                pre_ref[...] = compose(pre_ref[...], subs_ref[k])

        @pl.when(jnp.logical_not(opening_chip))
        def _():
            to_other.start()
            run_ref[...] = compose(pre_ref[...], core_ref[...])

        @pl.when(opening_chip)
        def _():
            run_ref[...] = identity(state)

        @pl.when(sub == 0)
        def _():
            majors_ref[plane] = chain([subs_ref[k] for k in range(n_sub)])

            @pl.when(plane != home)
            def _():
                to_head.start()

            @pl.when(plane == home)
            def _():
                others = majors_ref.at[pl.ds(0, planes - 1)]
                copy(others, others, column_send, majors_recv, place()).wait_recv()
                ahead_ref[0] = majors_ref[0]
                for k in range(1, planes):
                    ahead_ref[k] = compose(ahead_ref[k - 1], majors_ref[k])

    @pl.when(other)
    def _():
        @pl.when(origin)
        def _():
            run_ref[...] = identity(state)

        @pl.when(jnp.logical_not(origin))
        def _():
            to_lead.wait_send()
            to_other.wait_recv()
            run_ref[...] = pre_ref[...]

    coords, momenta = twice(run_ref[...])
    coords, momenta = with_tail(coords, -start_q), with_tail(momenta, -start_p)
    momenta = momenta - kick(coords, open_ref[...])

    def advance(t, carry):
        coords, momenta = carry
        coords = coords + step_size * momenta
        pair = kick(coords, kicks_ref[t])
        row = pl.ds(t, 1)
        maps_ref[t] = join(
            with_tail(coords, rows_ref[0, row, :]),
            with_tail(momenta - pair[:, state:], rows_ref[1, row, :]),
        )
        return (
            with_tail(coords, offs_ref[0, row, :]),
            with_tail(momenta - pair[:, :state], offs_ref[1, row, :]),
        )

    lax.fori_loop(0, steps - 1, advance, (coords, momenta))

    to_next = copy(
        vector_ref.at[onward], vector_ref.at[entry], column_send, state_recv,
        place((group + 1) * planes + home),
    )

    def to_plane(k):
        return copy(
            vector_ref.at[k], vector_ref.at[arrived], spread_send, state_recv,
            place(group * planes + k),
        )

    def to_device(at):
        return copy(
            vector_ref.at[arrived], vector_ref.at[arrived], spread_send, state_recv,
            place(tm, at // n_inner, at % n_inner),
        )

    def spread():
        for at in range(around):
            if at != last:
                to_device(at).start()

    def stand_at(slot):
        upright_ref[...] = jnp.broadcast_to(stand(vector_ref[slot]), (state, state))

    @pl.when(starts)
    def _():
        copy(guess_ref, raw_ref, spread_send, state_recv, place(0, 0, 0)).wait_recv()
        left = left_state(weights, raw_ref[...], start_ref[...])
        upright_ref[...] = jnp.broadcast_to(left, (state, state))

    @pl.when(head)
    def _():
        @pl.when(group > 0)
        def _():
            to_next.wait_recv()
            stand_at(entry)

        for k in range(planes):
            slot = k + 1 if k + 1 < planes else onward
            vector_ref[arrived if slot == home else slot] = laid(upright_ref[...], ahead_ref[k])

        @pl.when(group < n_groups - 1)
        def _():
            to_next.start()

        for k in range(1, planes):
            if k != home:
                to_plane(k).start()

        @pl.when(group > 0)
        def _():
            to_plane(0).start()

        spread()
        stand_at(arrived)

    @pl.when(both(tm > 0, jnp.logical_not(head)))
    def _():
        to_device(0).wait_recv()

        @pl.when(column)
        def _():
            spread()

        stand_at(arrived)

    upright = upright_ref[...]
    for t in range(steps):
        ref = run_ref if t == 0 else maps_ref.at[t - 1]
        out_ref[t : t + 1, :] = laid(upright, ref)

    def spread_left(rows):
        sent = maps_ref.at[0, pl.ds(0, rows), :]
        copy(sent, sent, spread_send, state_recv, place()).wait_send()

    @pl.when(origin)
    def _():
        spread_left(around * steps)

    @pl.when(lead)
    def _():
        for k in range(1, n_sub):
            @pl.when(given == k)
            def _():
                some_subs(k).wait_send()

        @pl.when(jnp.logical_not(opening_chip))
        def _():
            to_other.wait_send()

        @pl.when(jnp.logical_and(column, plane != home))
        def _():
            to_head.wait_send()

    @pl.when(both(head, group > 0))
    def _():
        spread_left(planes + around - 2)

    @pl.when(both(head, group == 0))
    def _():
        spread_left(planes + around - 3)

    @pl.when(both(column, tm > 0, plane != home))
    def _():
        spread_left(around - 1)

    @pl.when(both(head, group < n_groups - 1))
    def _():
        to_next.wait_send()


def shards(sizes, guess, start, layer_weight, layer_bias, amplitude):
    n_tm, n_sub, n_inner = sizes
    steps, state = guess.shape
    rows = state + tail
    hidden = layer_bias.shape[0]
    vmem = pl.BlockSpec(memory_space=pltpu.VMEM)
    dma = pltpu.SemaphoreType.DMA
    return pl.pallas_call(
        functools.partial(kernel, sizes),
        out_shape=pltpu.VMEM((steps, state), f32),
        in_specs=[pl.BlockSpec(memory_space=pl.ANY)] * 5,
        out_specs=vmem,
        scratch_shapes=[
            pltpu.VMEM((steps, state), f32),
            pltpu.VMEM((1, state), f32),
            pltpu.VMEM((state // 2, hidden), f32),
            pltpu.VMEM((1, hidden), f32),
            pltpu.VMEM((1, hidden), f32),
            pltpu.VMEM((steps, 2 * state, 2 * state), bf16),
            pltpu.VMEM((2 * state, state), bf16),
            pltpu.VMEM((2, steps, state), f32),
            pltpu.VMEM((2, steps, state), f32),
            pltpu.VMEM((rows, state), f32),
            pltpu.VMEM((n_sub, rows, state), f32),
            pltpu.VMEM((planes, rows, state), f32),
            pltpu.VMEM((planes, rows, state), f32),
            pltpu.VMEM((rows, state), f32),
            pltpu.VMEM((rows, state), f32),
            pltpu.VMEM((3 + planes, 1, state), f32),
            pltpu.VMEM((steps, rows, state), f32),
            pltpu.VMEM((2 * state, hidden), bf16),
            pltpu.VMEM((hidden, 2 * state), bf16),
            pltpu.VMEM((steps, state), f32),
            pltpu.VMEM((state, state), f32),
            dma,
            dma,
            dma,
            dma,
            dma,
            dma,
            dma,
            dma,
            dma,
            dma,
        ],
        compiler_params=pltpu.CompilerParams(collective_id=0, has_side_effects=True),
    )(guess, start.reshape(1, -1), layer_weight.T, layer_bias.reshape(1, -1), amplitude.reshape(1, -1))


def solution(mesh):
    sizes = tuple(mesh.shape[name] for name in ("tm", "sub", "inner"))
    placed = (P(("parts", "tm", "sub", "inner"), None), P("parts"), P(), P(), P())
    return jax.shard_map(
        functools.partial(shards, sizes),
        mesh=mesh,
        in_specs=placed,
        out_specs=P(("parts", "tm", "sub", "inner"), None),
        check_vma=False,
    )
```

```python
import functools

import jax
import jax.numpy as jnp
from jax import lax
from jax.experimental import pallas as pl
from jax.experimental.pallas import tpu as pltpu
from jax.sharding import PartitionSpec as P

step_size = 0.04
curvature = 0.5
half_step = 0.5 * step_size
f32, bf16 = jnp.float32, jnp.bfloat16
MESH = pl.DeviceIdType.MESH
planes = 4
home = 1
tail = 8


def iota(shape, axis):
    return lax.broadcasted_iota(jnp.int32, shape, axis)


def split(value):
    high = value.astype(bf16)
    return high, (value - high.astype(f32)).astype(bf16)


def low_lanes(value):
    width = value.shape[-1]
    return iota(value.shape, 1) < width // 2


def mixed(value):
    high = value.astype(bf16).astype(f32)
    return jnp.where(low_lanes(value), high, value - high).astype(bf16)


def twice(value):
    swapped = pltpu.roll(value, value.shape[-1] // 2, 1)
    low = low_lanes(value)
    return jnp.where(low, value, swapped), jnp.where(low, swapped, value)


def join(coords, momenta):
    return jnp.where(low_lanes(coords), coords, momenta)


def dot(left, right):
    return jnp.dot(left, right, preferred_element_type=f32)


def with_tail(value, extra):
    rows = value.shape[0] - tail
    if rows == 0:
        return value + extra
    return jnp.concatenate([value[:rows], value[rows:] + extra], axis=0)


def compose(first, second):
    state = first.shape[1]
    eye = (iota((state, state), 0) == iota((state, state), 1)).astype(f32)
    high, low = split(second[:state] - eye)
    both = jnp.concatenate([high, low], axis=1)
    left = jnp.concatenate(split(first), axis=1)
    out = dot(left, jnp.concatenate([both, both], axis=0))
    return with_tail(first + (out[:, :state] + out[:, state:]), second[state:])


def chain(maps):
    while len(maps) > 1:
        maps = [
            compose(maps[k], maps[k + 1]) if k + 1 < len(maps) else maps[k]
            for k in range(0, len(maps), 2)
        ]
    return maps[0]


def identity(state):
    rows = state + tail
    return (iota((rows, state), 0) == iota((rows, state), 1)).astype(f32)


def diagonal_mask(state):
    return iota((state, state), 0) == iota((state, state), 1)


def stand(row):
    return jnp.sum(jnp.where(diagonal_mask(row.shape[1]), row, 0.0), axis=1, keepdims=True)


def laid(column, full):
    state = full.shape[1]
    return jnp.sum(column * full[:state], axis=0, keepdims=True) + full[state : state + 1]


def stood(row, full):
    state = full.shape[1]
    shift = jnp.where(diagonal_mask(state), full[state : state + 1], 0.0)
    return jnp.sum(full[:state].T * row + shift, axis=1, keepdims=True)


class Weights:
    def __init__(self, across_ref, onto_ref, back_ref, bias_ref, amplitude_ref):
        self.across_ref, self.onto_ref, self.back_ref = across_ref, onto_ref, back_ref
        self.bias_ref, self.amplitude_ref = bias_ref, amplitude_ref

    def fill(self, weight):
        across = jnp.concatenate([weight, weight], axis=0)
        high, low = split(across)
        self.onto_ref[...] = jnp.concatenate([high, low], axis=0)
        high, low = split(across.T)
        self.back_ref[...] = jnp.concatenate([high, low], axis=1)

    def along(self, value):
        left = mixed(value)
        return dot(jnp.concatenate([left, left], axis=1), self.onto_ref[...])

    def apart(self, value):
        back = self.back_ref[...]
        state, rows = back.shape[1] // 2, value.shape[0]
        out = dot(jnp.concatenate(split(value), axis=0), back)
        out = out[:rows] + out[rows:]
        return out[:, :state] + out[:, state:]

    def forces(self, coords):
        gate = 1.0 / (1.0 + jnp.exp(-(self.along(coords) + self.bias_ref[...])))
        pull = self.amplitude_ref[...] * gate
        return self.apart(pull) + curvature * coords, pull * (1.0 - gate)

    def hessians(self, curves, diagonal):
        count = curves.shape[0]
        across, back = self.across_ref[...], self.back_ref[...]
        width, state = across.shape[0], back.shape[1] // 2
        parts = [split(across * curves[k : k + 1]) for k in range(count)]
        stacked = jnp.concatenate([p[0] for p in parts] + [p[1] for p in parts], axis=0)
        out = dot(stacked, back)
        out = out[:, :state] + out[:, state:]
        out = out[: count * width] + out[count * width :]
        unit = jnp.where(iota((width, state), 0) == iota((width, state), 1) % width, 1.0, 0.0)
        return [out[k * width : (k + 1) * width] + diagonal[k] * unit for k in range(count)]


def stationary(hessian):
    high, low = split(hessian)
    return jnp.concatenate([high, high, low, low], axis=0)


class Window:
    def __init__(self, weights, rows, start):
        self.steps, self.state = steps, state = rows.shape
        coords, momenta = twice(
            jnp.concatenate([rows, jnp.broadcast_to(start, (tail, state))], axis=0)
        )
        grad_zero, curve_zero = weights.forces(coords)
        half = momenta - half_step * grad_zero
        moved = coords + step_size * half
        grad_one, curve_one = weights.forces(moved)
        landed = half - half_step * grad_one
        self.first_q, self.first_p = moved[steps:], landed[steps:]
        self.first = join(self.first_q, self.first_p)[:1]
        coords, momenta = coords[:steps], momenta[:steps]
        self.curve_zero, self.curve_one = curve_zero[:steps], curve_one[:steps]
        self.moved, self.landed = moved[:steps], landed[:steps]
        self.start_q, self.start_p = coords[:1], momenta[:1]
        inside = iota((steps, 1), 0) < steps - 1

        def later(value):
            return jnp.where(inside, pltpu.roll(value, steps - 1, 0), 0.0)

        curve_next = later(self.curve_zero)
        opening = jnp.broadcast_to(self.curve_zero[:1], (tail, self.curve_zero.shape[1]))
        self.curves = jnp.concatenate([self.curve_one + curve_next, opening], axis=0)[: steps + 1]
        self.diagonal = [2.0 * curvature] * (steps - 1) + [curvature, curvature]
        self.off_q = self.moved - later(coords)
        begin_q = self.first_q - self.start_q
        begin_p = self.first_p - self.start_p
        pulled = jnp.concatenate([jnp.where(inside, self.off_q, 0.0), begin_q], axis=0)
        curve = jnp.concatenate([curve_next, opening], axis=0)
        kicked = half_step * (weights.apart(weights.along(pulled) * curve) + curvature * pulled)
        self.off_p = self.landed - later(momenta) - kicked[:steps]
        self.begin_q, self.begin_p = begin_q, begin_p - kicked[steps:]


def kick(coords, kicks):
    left = mixed(coords)
    return half_step * dot(jnp.concatenate([left, left], axis=1), kicks)


def window_map(window, kicks):
    steps, state = window.steps, window.state
    runs = 4
    length = steps // runs
    ident = identity(state)
    states = []
    for c in range(runs):
        coords, momenta = twice(ident)
        if c == 0:
            coords = with_tail(coords, -window.start_q)
            momenta = with_tail(momenta, -window.start_p)
            momenta = momenta - kick(coords, kicks[steps])
        states.append((coords, momenta))
    for j in range(length):
        for c in range(runs):
            t = c * length + j
            coords, momenta = states[c]
            coords = coords + step_size * momenta
            momenta = momenta - kick(coords, kicks[t])
            states[c] = (
                with_tail(coords, window.off_q[t : t + 1]),
                with_tail(momenta, window.off_p[t : t + 1]),
            )
    return chain([join(*s) for s in states])


def run_lengths(steps):
    short = steps // 8
    found = [short, short] + [(steps - 2 * short) // 4] * 4
    return found[:-1] + [steps - sum(found[:-1])]


def left_state(weights, rows, start):
    window = Window(weights, rows, start)
    steps, state = window.steps, window.state
    width = state // 2
    lengths = run_lengths(steps)
    begins = [sum(lengths[:c]) for c in range(len(lengths))]
    hessians = weights.hessians(window.curves[:steps], window.diagonal)
    repeated = jnp.where(iota((width, state), 0) == iota((width, state), 1) % width, 1.0, 0.0)
    none = jnp.zeros((tail, state), f32)
    moving = jnp.concatenate([repeated, step_size * repeated, none], axis=0)
    states = [(window.begin_q, window.begin_p)]
    for t in begins[1:]:
        bend = half_step * hessians[t]
        momenta = jnp.concatenate([-bend, repeated - step_size * bend, none], axis=0)
        states.append((
            with_tail(moving, window.off_q[t : t + 1]),
            with_tail(momenta, window.off_p[t : t + 1]),
        ))
    for j in range(max(lengths)):
        for c, length in enumerate(lengths):
            t = begins[c] + j + (1 if c else 0)
            if t >= begins[c] + length:
                continue
            coords, momenta = states[c]
            coords = coords + step_size * momenta
            momenta = momenta - kick(coords, stationary(hessians[t]))
            states[c] = (
                with_tail(coords, window.off_q[t : t + 1]),
                with_tail(momenta, window.off_p[t : t + 1]),
            )
    maps = [join(*s) for s in states]
    vector, upright = maps[0][:1], False
    for full in maps[1:]:
        vector = laid(vector, full) if upright else stood(vector, full)
        upright = not upright
    return vector if upright else stand(vector)


def kernel(
    sizes, guess_hbm, start_hbm, weight_hbm, bias_hbm, amplitude_hbm, out_ref,
    guess_ref, start_ref, weight_ref, bias_ref, amplitude_ref,
    kicks_ref, open_ref, offs_ref, rows_ref, core_ref, subs_ref, majors_ref, ahead_ref,
    pre_ref, run_ref, vector_ref, maps_ref, onto_ref, back_ref, raw_ref,
    upright_ref, pair_send, pair_recv, subs_send, subs_recv, column_send, majors_recv,
    spread_send, state_recv, load_guess, load_last,
):
    n_tm, n_sub, n_inner = sizes
    n_groups = n_tm // planes
    part, tm = lax.axis_index("parts"), lax.axis_index("tm")
    sub, inner = lax.axis_index("sub"), lax.axis_index("inner")
    group, plane = lax.div(tm, planes), lax.rem(tm, planes)
    steps, state = guess_ref.shape
    last = n_inner - 1
    lead = inner == last
    other = jnp.logical_not(lead)
    column = jnp.logical_and(lead, sub == 0)
    head = jnp.logical_and(column, plane == home)
    opening_chip = jnp.logical_and(tm == 0, sub == 0)
    origin = jnp.logical_and(opening_chip, inner == 0)
    starts = jnp.logical_and(
        jnp.logical_not(origin), jnp.logical_or(tm == 0, jnp.logical_and(head, group == 0))
    )

    def place(tm_at=None, sub_at=None, inner_at=None):
        return (
            part,
            tm if tm_at is None else tm_at,
            sub if sub_at is None else sub_at,
            inner if inner_at is None else inner_at,
        )

    def copy(source, target, send, recv, where):
        return pltpu.make_async_remote_copy(
            src_ref=source, dst_ref=target, send_sem=send, recv_sem=recv,
            device_id=where, device_id_type=MESH,
        )

    def both(*conditions):
        return functools.reduce(jnp.logical_and, conditions)

    barrier = pltpu.get_barrier_semaphore()
    around = n_sub * n_inner
    loads = [
        pltpu.make_async_copy(source, target, sem)
        for source, target, sem in (
            (guess_hbm, guess_ref, load_guess), (weight_hbm, weight_ref, subs_send),
            (start_hbm, start_ref, column_send), (bias_hbm, bias_ref, pair_send),
            (amplitude_hbm, amplitude_ref, load_last),
        )
    ]
    loads[0].start()

    def from_origin(at):
        where = place(0, at // n_inner, at % n_inner) if at < around else place(home, 0, last)
        return copy(guess_ref, raw_ref, spread_send, state_recv, where)

    @pl.when(origin)
    def _():
        pl.semaphore_wait(barrier, around)
        loads[0].wait()
        for at in range(1, around + 1):
            from_origin(at).start()

    for load in loads[1:]:
        load.start()

    @pl.when(jnp.logical_not(origin))
    def _():
        loads[0].wait()

    def greet(where):
        pl.semaphore_signal(barrier, inc=1, device_id=where, device_id_type=MESH)

    @pl.when(jnp.logical_not(origin))
    def _():
        @pl.when(jnp.logical_not(both(opening_chip, lead)))
        def _():
            greet(place(inner_at=n_inner - 1 - inner))

        @pl.when(starts)
        def _():
            greet(place(0, 0, 0))

        @pl.when(both(tm > 0, jnp.logical_not(column)))
        def _():
            greet(place(tm, 0, last))

        @pl.when(both(column, tm > 0, plane != home))
        def _():
            greet(place(group * planes + home))

    def takes_from(s):
        return both(lead, sub != s, jnp.logical_or(sub > s, sub == 0))

    def gives_to(t):
        return both(lead, sub != t, jnp.logical_or(sub < t, t == 0))

    for s in range(n_sub):
        @pl.when(takes_from(s))
        def _():
            greet(place(sub_at=s))

    @pl.when(head)
    def _():
        for k in range(planes):
            if k != home:
                greet(place(group * planes + k))

        @pl.when(group > 0)
        def _():
            greet(place((group - 1) * planes + home))

    for load in loads[1:]:
        load.wait()
    weights = Weights(weight_ref, onto_ref, back_ref, bias_ref, amplitude_ref)
    weights.fill(weight_ref[...])
    start = start_ref[...]
    window = Window(weights, guess_ref[...], start)
    found = [stationary(k) for k in weights.hessians(window.curves, window.diagonal)]
    run_ref[...] = window_map(window, found)
    start_q, start_p = window.start_q, window.start_p

    count = jnp.where(jnp.logical_and(lead, jnp.logical_not(opening_chip)), 1, 0)
    count = count + jnp.where(other, 1, 0)
    count = count + jnp.where(lead, jnp.where(sub == 0, n_sub - 1, n_sub - sub), 0)
    count = count + jnp.where(jnp.logical_and(column, plane != home), 1, 0)
    count = count + jnp.where(head, jnp.where(group > 0, planes - 1, planes - 2), 0)
    count = count + jnp.where(jnp.logical_and(column, tm > 0), around - 1, 0)
    count = count + jnp.where(jnp.logical_and(head, group < n_groups - 1), 1, 0)

    @pl.when(jnp.logical_not(origin))
    def _():
        pl.semaphore_wait(barrier, count)

    entry, arrived, onward = 0, planes + 1, planes + 2

    @pl.when(origin)
    def _():
        upright_ref[...] = jnp.broadcast_to(stand(window.first), (state, state))

    for t in range(steps):
        kicks_ref[t, :, :state] = found[t]
    open_ref[...] = found[steps]
    offs_ref[0] = window.off_q
    offs_ref[1] = window.off_p
    rows_ref[0] = window.moved
    rows_ref[1] = window.landed
    plain = weights.hessians(window.curve_one, [curvature] * steps)
    for t in range(steps):
        kicks_ref[t, :, state:] = stationary(plain[t])

    to_lead = copy(run_ref, core_ref, pair_send, pair_recv, place(inner_at=last))
    to_other = copy(pre_ref, pre_ref, pair_send, pair_recv, place(inner_at=0))
    to_head = copy(
        majors_ref.at[plane], majors_ref.at[plane], column_send, majors_recv,
        place(group * planes + home),
    )

    def to_sub(t):
        return copy(
            subs_ref.at[sub], subs_ref.at[sub], subs_send, subs_recv, place(sub_at=t)
        )

    def some_subs(count):
        part_of = subs_ref.at[pl.ds(0, count)]
        return copy(part_of, part_of, subs_send, subs_recv, place())

    given = jnp.where(sub == 0, n_sub - 1, n_sub - sub)
    taken = jnp.where(sub == 0, n_sub - 1, sub)

    @pl.when(jnp.logical_and(other, jnp.logical_not(origin)))
    def _():
        to_lead.start()

    @pl.when(lead)
    def _():
        @pl.when(opening_chip)
        def _():
            subs_ref[sub] = run_ref[...]

        @pl.when(jnp.logical_not(opening_chip))
        def _():
            to_lead.wait_recv()
            subs_ref[sub] = compose(core_ref[...], run_ref[...])

        for t in range(n_sub):
            @pl.when(gives_to(t))
            def _():
                to_sub(t).start()

        for k in range(1, n_sub):
            @pl.when(taken == k)
            def _():
                some_subs(k).wait_recv()

        pre_ref[...] = identity(state)
        for k in range(n_sub - 1):
            @pl.when(k < sub)
            def _():
                pre_ref[...] = compose(pre_ref[...], subs_ref[k])

        @pl.when(jnp.logical_not(opening_chip))
        def _():
            to_other.start()
            run_ref[...] = compose(pre_ref[...], core_ref[...])

        @pl.when(opening_chip)
        def _():
            run_ref[...] = identity(state)

        @pl.when(sub == 0)
        def _():
            majors_ref[plane] = chain([subs_ref[k] for k in range(n_sub)])

            @pl.when(plane != home)
            def _():
                to_head.start()

            @pl.when(plane == home)
            def _():
                others = majors_ref.at[pl.ds(0, planes - 1)]
                copy(others, others, column_send, majors_recv, place()).wait_recv()
                ahead_ref[0] = majors_ref[0]
                for k in range(1, planes):
                    ahead_ref[k] = compose(ahead_ref[k - 1], majors_ref[k])

    @pl.when(other)
    def _():
        @pl.when(origin)
        def _():
            run_ref[...] = identity(state)

        @pl.when(jnp.logical_not(origin))
        def _():
            to_lead.wait_send()
            to_other.wait_recv()
            run_ref[...] = pre_ref[...]

    coords, momenta = twice(run_ref[...])
    coords, momenta = with_tail(coords, -start_q), with_tail(momenta, -start_p)
    momenta = momenta - kick(coords, open_ref[...])

    def advance(t, carry):
        coords, momenta = carry
        coords = coords + step_size * momenta
        pair = kick(coords, kicks_ref[t])
        row = pl.ds(t, 1)
        maps_ref[t] = join(
            with_tail(coords, rows_ref[0, row, :]),
            with_tail(momenta - pair[:, state:], rows_ref[1, row, :]),
        )
        return (
            with_tail(coords, offs_ref[0, row, :]),
            with_tail(momenta - pair[:, :state], offs_ref[1, row, :]),
        )

    lax.fori_loop(0, steps - 1, advance, (coords, momenta))

    to_next = copy(
        vector_ref.at[onward], vector_ref.at[entry], column_send, state_recv,
        place((group + 1) * planes + home),
    )

    def to_plane(k):
        return copy(
            vector_ref.at[k], vector_ref.at[arrived], spread_send, state_recv,
            place(group * planes + k),
        )

    def to_device(at):
        return copy(
            vector_ref.at[arrived], vector_ref.at[arrived], spread_send, state_recv,
            place(tm, at // n_inner, at % n_inner),
        )

    def spread():
        for at in range(around):
            if at != last:
                to_device(at).start()

    def stand_at(slot):
        upright_ref[...] = jnp.broadcast_to(stand(vector_ref[slot]), (state, state))

    @pl.when(starts)
    def _():
        copy(guess_ref, raw_ref, spread_send, state_recv, place(0, 0, 0)).wait_recv()
        left = left_state(weights, raw_ref[...], start_ref[...])
        upright_ref[...] = jnp.broadcast_to(left, (state, state))

    @pl.when(head)
    def _():
        @pl.when(group > 0)
        def _():
            to_next.wait_recv()
            stand_at(entry)

        for k in range(planes):
            slot = k + 1 if k + 1 < planes else onward
            vector_ref[arrived if slot == home else slot] = laid(upright_ref[...], ahead_ref[k])

        @pl.when(group < n_groups - 1)
        def _():
            to_next.start()

        for k in range(1, planes):
            if k != home:
                to_plane(k).start()

        @pl.when(group > 0)
        def _():
            to_plane(0).start()

        spread()
        stand_at(arrived)

    @pl.when(both(tm > 0, jnp.logical_not(head)))
    def _():
        to_device(0).wait_recv()

        @pl.when(column)
        def _():
            spread()

        stand_at(arrived)

    upright = upright_ref[...]
    for t in range(steps):
        ref = run_ref if t == 0 else maps_ref.at[t - 1]
        out_ref[t : t + 1, :] = laid(upright, ref)

    def spread_left(rows):
        sent = maps_ref.at[0, pl.ds(0, rows), :]
        copy(sent, sent, spread_send, state_recv, place()).wait_send()

    @pl.when(origin)
    def _():
        spread_left(around * steps)

    @pl.when(lead)
    def _():
        for k in range(1, n_sub):
            @pl.when(given == k)
            def _():
                some_subs(k).wait_send()

        @pl.when(jnp.logical_not(opening_chip))
        def _():
            to_other.wait_send()

        @pl.when(jnp.logical_and(column, plane != home))
        def _():
            to_head.wait_send()

    @pl.when(both(head, group > 0))
    def _():
        spread_left(planes + around - 2)

    @pl.when(both(head, group == 0))
    def _():
        spread_left(planes + around - 3)

    @pl.when(both(column, tm > 0, plane != home))
    def _():
        spread_left(around - 1)

    @pl.when(both(head, group < n_groups - 1))
    def _():
        to_next.wait_send()


def shards(sizes, guess, start, layer_weight, layer_bias, amplitude):
    n_tm, n_sub, n_inner = sizes
    steps, state = guess.shape
    rows = state + tail
    hidden = layer_bias.shape[0]
    vmem = pl.BlockSpec(memory_space=pltpu.VMEM)
    dma = pltpu.SemaphoreType.DMA
    return pl.pallas_call(
        functools.partial(kernel, sizes),
        out_shape=pltpu.VMEM((steps, state), f32),
        in_specs=[pl.BlockSpec(memory_space=pl.ANY)] * 5,
        out_specs=vmem,
        scratch_shapes=[
            pltpu.VMEM((steps, state), f32),
            pltpu.VMEM((1, state), f32),
            pltpu.VMEM((state // 2, hidden), f32),
            pltpu.VMEM((1, hidden), f32),
            pltpu.VMEM((1, hidden), f32),
            pltpu.VMEM((steps, 2 * state, 2 * state), bf16),
            pltpu.VMEM((2 * state, state), bf16),
            pltpu.VMEM((2, steps, state), f32),
            pltpu.VMEM((2, steps, state), f32),
            pltpu.VMEM((rows, state), f32),
            pltpu.VMEM((n_sub, rows, state), f32),
            pltpu.VMEM((planes, rows, state), f32),
            pltpu.VMEM((planes, rows, state), f32),
            pltpu.VMEM((rows, state), f32),
            pltpu.VMEM((rows, state), f32),
            pltpu.VMEM((3 + planes, 1, state), f32),
            pltpu.VMEM((steps, rows, state), f32),
            pltpu.VMEM((2 * state, hidden), bf16),
            pltpu.VMEM((hidden, 2 * state), bf16),
            pltpu.VMEM((steps, state), f32),
            pltpu.VMEM((state, state), f32),
            dma,
            dma,
            dma,
            dma,
            dma,
            dma,
            dma,
            dma,
            dma,
            dma,
        ],
        compiler_params=pltpu.CompilerParams(collective_id=0, has_side_effects=True),
    )(guess, start.reshape(1, -1), layer_weight.T, layer_bias.reshape(1, -1), amplitude.reshape(1, -1))


def solution(mesh):
    sizes = tuple(mesh.shape[name] for name in ("tm", "sub", "inner"))
    placed = (P(("parts", "tm", "sub", "inner"), None), P("parts"), P(), P(), P())
    return jax.shard_map(
        functools.partial(shards, sizes),
        mesh=mesh,
        in_specs=placed,
        out_specs=P(("parts", "tm", "sub", "inner"), None),
        check_vma=False,
    )
```

```python
import functools

import jax
import jax.numpy as jnp
from jax import lax
from jax.experimental import pallas as pl
from jax.experimental.pallas import tpu as pltpu
from jax.sharding import PartitionSpec as P

step_size = 0.04
curvature = 0.5
half_step = 0.5 * step_size
f32, bf16 = jnp.float32, jnp.bfloat16
MESH = pl.DeviceIdType.MESH
planes = 4
home = 1
tail = 8


def iota(shape, axis):
    return lax.broadcasted_iota(jnp.int32, shape, axis)


def split(value):
    high = value.astype(bf16)
    return high, (value - high.astype(f32)).astype(bf16)


def thirds(value):
    high, rest = value.astype(bf16), value - value.astype(bf16).astype(f32)
    return (high, *split(rest))


def low_lanes(value):
    width = value.shape[-1]
    return iota(value.shape, 1) < width // 2


def mixed(value):
    high = value.astype(bf16).astype(f32)
    return jnp.where(low_lanes(value), high, value - high).astype(bf16)


def twice(value):
    swapped = pltpu.roll(value, value.shape[-1] // 2, 1)
    low = low_lanes(value)
    return jnp.where(low, value, swapped), jnp.where(low, swapped, value)


def join(coords, momenta):
    return jnp.where(low_lanes(coords), coords, momenta)


def dot(left, right):
    return jnp.dot(left, right, preferred_element_type=f32)


def with_tail(value, extra):
    rows = value.shape[0] - tail
    if rows == 0:
        return value + extra
    return jnp.concatenate([value[:rows], value[rows:] + extra], axis=0)


def compose(first, second):
    state = first.shape[1]
    eye = (iota((state, state), 0) == iota((state, state), 1)).astype(f32)
    high, middle, low = thirds(second[:state] - eye)
    both = jnp.concatenate([high, middle], axis=1)
    high_left, middle_left, low_left = thirds(first)
    left = jnp.concatenate([high_left, middle_left], axis=1)
    out = dot(left, jnp.concatenate([both, both], axis=0))
    left = jnp.concatenate([high_left, low_left], axis=1)
    small = dot(left, jnp.concatenate([low, high], axis=0))
    return with_tail(first + (out[:, :state] + (out[:, state:] + small)), second[state:])


def chain(maps):
    while len(maps) > 1:
        maps = [
            compose(maps[k], maps[k + 1]) if k + 1 < len(maps) else maps[k]
            for k in range(0, len(maps), 2)
        ]
    return maps[0]


def identity(state):
    rows = state + tail
    return (iota((rows, state), 0) == iota((rows, state), 1)).astype(f32)


def diagonal_mask(state):
    return iota((state, state), 0) == iota((state, state), 1)


def stand(row):
    return jnp.sum(jnp.where(diagonal_mask(row.shape[1]), row, 0.0), axis=1, keepdims=True)


def laid(column, full):
    state = full.shape[1]
    return jnp.sum(column * full[:state], axis=0, keepdims=True) + full[state : state + 1]


def stood(row, full):
    state = full.shape[1]
    shift = jnp.where(diagonal_mask(state), full[state : state + 1], 0.0)
    return jnp.sum(full[:state].T * row + shift, axis=1, keepdims=True)


class Weights:
    def __init__(self, across_ref, onto_ref, back_ref, bias_ref, amplitude_ref):
        self.across_ref, self.onto_ref, self.back_ref = across_ref, onto_ref, back_ref
        self.bias_ref, self.amplitude_ref = bias_ref, amplitude_ref

    def fill(self, weight):
        across = jnp.concatenate([weight, weight], axis=0)
        high, low = split(across)
        self.onto_ref[...] = jnp.concatenate([high, low], axis=0)
        high, low = split(across.T)
        self.back_ref[...] = jnp.concatenate([high, low], axis=1)

    def along(self, value):
        left = mixed(value)
        return dot(jnp.concatenate([left, left], axis=1), self.onto_ref[...])

    def apart(self, value):
        back = self.back_ref[...]
        state, rows = back.shape[1] // 2, value.shape[0]
        out = dot(jnp.concatenate(split(value), axis=0), back)
        out = out[:rows] + out[rows:]
        return out[:, :state] + out[:, state:]

    def forces(self, coords):
        gate = 1.0 / (1.0 + jnp.exp(-(self.along(coords) + self.bias_ref[...])))
        pull = self.amplitude_ref[...] * gate
        return self.apart(pull) + curvature * coords, pull * (1.0 - gate)

    def hessians(self, curves, diagonal):
        count = curves.shape[0]
        across, back = self.across_ref[...], self.back_ref[...]
        width, state = across.shape[0], back.shape[1] // 2
        parts = [split(across * curves[k : k + 1]) for k in range(count)]
        stacked = jnp.concatenate([p[0] for p in parts] + [p[1] for p in parts], axis=0)
        out = dot(stacked, back)
        out = out[:, :state] + out[:, state:]
        out = out[: count * width] + out[count * width :]
        unit = jnp.where(iota((width, state), 0) == iota((width, state), 1) % width, 1.0, 0.0)
        return [out[k * width : (k + 1) * width] + diagonal[k] * unit for k in range(count)]


def stationary(hessian):
    high, low = split(hessian)
    return jnp.concatenate([high, high, low, low], axis=0)


class Window:
    def __init__(self, weights, rows, start):
        self.steps, self.state = steps, state = rows.shape
        coords, momenta = twice(
            jnp.concatenate([rows, jnp.broadcast_to(start, (tail, state))], axis=0)
        )
        grad_zero, curve_zero = weights.forces(coords)
        half = momenta - half_step * grad_zero
        moved = coords + step_size * half
        grad_one, curve_one = weights.forces(moved)
        landed = half - half_step * grad_one
        self.first_q, self.first_p = moved[steps:], landed[steps:]
        self.first = join(self.first_q, self.first_p)[:1]
        coords, momenta = coords[:steps], momenta[:steps]
        self.curve_zero, self.curve_one = curve_zero[:steps], curve_one[:steps]
        self.moved, self.landed = moved[:steps], landed[:steps]
        self.start_q, self.start_p = coords[:1], momenta[:1]
        inside = iota((steps, 1), 0) < steps - 1

        def later(value):
            return jnp.where(inside, pltpu.roll(value, steps - 1, 0), 0.0)

        curve_next = later(self.curve_zero)
        opening = jnp.broadcast_to(self.curve_zero[:1], (tail, self.curve_zero.shape[1]))
        self.curves = jnp.concatenate([self.curve_one + curve_next, opening], axis=0)[: steps + 1]
        self.diagonal = [2.0 * curvature] * (steps - 1) + [curvature, curvature]
        self.off_q = self.moved - later(coords)
        begin_q = self.first_q - self.start_q
        begin_p = self.first_p - self.start_p
        pulled = jnp.concatenate([jnp.where(inside, self.off_q, 0.0), begin_q], axis=0)
        curve = jnp.concatenate([curve_next, opening], axis=0)
        kicked = half_step * (weights.apart(weights.along(pulled) * curve) + curvature * pulled)
        self.off_p = self.landed - later(momenta) - kicked[:steps]
        self.begin_q, self.begin_p = begin_q, begin_p - kicked[steps:]


def kick(coords, kicks):
    left = mixed(coords)
    return half_step * dot(jnp.concatenate([left, left], axis=1), kicks)


def window_map(window, kicks):
    steps, state = window.steps, window.state
    runs = 4
    length = steps // runs
    ident = identity(state)
    states = []
    for c in range(runs):
        coords, momenta = twice(ident)
        if c == 0:
            coords = with_tail(coords, -window.start_q)
            momenta = with_tail(momenta, -window.start_p)
            momenta = momenta - kick(coords, kicks[steps])
        states.append((coords, momenta))
    for j in range(length):
        for c in range(runs):
            t = c * length + j
            coords, momenta = states[c]
            coords = coords + step_size * momenta
            momenta = momenta - kick(coords, kicks[t])
            states[c] = (
                with_tail(coords, window.off_q[t : t + 1]),
                with_tail(momenta, window.off_p[t : t + 1]),
            )
    return chain([join(*s) for s in states])


def run_lengths(steps):
    short = steps // 8
    found = [short, short] + [(steps - 2 * short) // 4] * 4
    return found[:-1] + [steps - sum(found[:-1])]


def left_state(weights, rows, start):
    window = Window(weights, rows, start)
    steps, state = window.steps, window.state
    width = state // 2
    lengths = run_lengths(steps)
    begins = [sum(lengths[:c]) for c in range(len(lengths))]
    hessians = weights.hessians(window.curves[:steps], window.diagonal)
    repeated = jnp.where(iota((width, state), 0) == iota((width, state), 1) % width, 1.0, 0.0)
    none = jnp.zeros((tail, state), f32)
    moving = jnp.concatenate([repeated, step_size * repeated, none], axis=0)
    states = [(window.begin_q, window.begin_p)]
    for t in begins[1:]:
        bend = half_step * hessians[t]
        momenta = jnp.concatenate([-bend, repeated - step_size * bend, none], axis=0)
        states.append((
            with_tail(moving, window.off_q[t : t + 1]),
            with_tail(momenta, window.off_p[t : t + 1]),
        ))
    for j in range(max(lengths)):
        for c, length in enumerate(lengths):
            t = begins[c] + j + (1 if c else 0)
            if t >= begins[c] + length:
                continue
            coords, momenta = states[c]
            coords = coords + step_size * momenta
            momenta = momenta - kick(coords, stationary(hessians[t]))
            states[c] = (
                with_tail(coords, window.off_q[t : t + 1]),
                with_tail(momenta, window.off_p[t : t + 1]),
            )
    maps = [join(*s) for s in states]
    vector, upright = maps[0][:1], False
    for full in maps[1:]:
        vector = laid(vector, full) if upright else stood(vector, full)
        upright = not upright
    return vector if upright else stand(vector)


def kernel(
    sizes, guess_hbm, start_hbm, weight_hbm, bias_hbm, amplitude_hbm, out_ref,
    guess_ref, start_ref, weight_ref, bias_ref, amplitude_ref,
    kicks_ref, open_ref, offs_ref, rows_ref, core_ref, subs_ref, majors_ref, ahead_ref,
    pre_ref, run_ref, vector_ref, maps_ref, onto_ref, back_ref, raw_ref,
    upright_ref, pair_send, pair_recv, subs_send, subs_recv, column_send, majors_recv,
    spread_send, state_recv, load_guess, load_last,
):
    n_tm, n_sub, n_inner = sizes
    n_groups = n_tm // planes
    part, tm = lax.axis_index("parts"), lax.axis_index("tm")
    sub, inner = lax.axis_index("sub"), lax.axis_index("inner")
    group, plane = lax.div(tm, planes), lax.rem(tm, planes)
    steps, state = guess_ref.shape
    last = n_inner - 1
    lead = inner == last
    other = jnp.logical_not(lead)
    column = jnp.logical_and(lead, sub == 0)
    head = jnp.logical_and(column, plane == home)
    opening_chip = jnp.logical_and(tm == 0, sub == 0)
    origin = jnp.logical_and(opening_chip, inner == 0)
    starts = jnp.logical_and(
        jnp.logical_not(origin), jnp.logical_or(tm == 0, jnp.logical_and(head, group == 0))
    )

    def place(tm_at=None, sub_at=None, inner_at=None):
        return (
            part,
            tm if tm_at is None else tm_at,
            sub if sub_at is None else sub_at,
            inner if inner_at is None else inner_at,
        )

    def copy(source, target, send, recv, where):
        return pltpu.make_async_remote_copy(
            src_ref=source, dst_ref=target, send_sem=send, recv_sem=recv,
            device_id=where, device_id_type=MESH,
        )

    def both(*conditions):
        return functools.reduce(jnp.logical_and, conditions)

    barrier = pltpu.get_barrier_semaphore()
    around = n_sub * n_inner
    loads = [
        pltpu.make_async_copy(source, target, sem)
        for source, target, sem in (
            (guess_hbm, guess_ref, load_guess), (weight_hbm, weight_ref, subs_send),
            (start_hbm, start_ref, column_send), (bias_hbm, bias_ref, pair_send),
            (amplitude_hbm, amplitude_ref, load_last),
        )
    ]
    loads[0].start()

    def from_origin(at):
        where = place(0, at // n_inner, at % n_inner) if at < around else place(home, 0, last)
        return copy(guess_ref, raw_ref, spread_send, state_recv, where)

    @pl.when(origin)
    def _():
        pl.semaphore_wait(barrier, around)
        loads[0].wait()
        for at in range(1, around + 1):
            from_origin(at).start()

    for load in loads[1:]:
        load.start()

    @pl.when(jnp.logical_not(origin))
    def _():
        loads[0].wait()

    def greet(where):
        pl.semaphore_signal(barrier, inc=1, device_id=where, device_id_type=MESH)

    @pl.when(jnp.logical_not(origin))
    def _():
        @pl.when(jnp.logical_not(both(opening_chip, lead)))
        def _():
            greet(place(inner_at=n_inner - 1 - inner))

        @pl.when(starts)
        def _():
            greet(place(0, 0, 0))

        @pl.when(both(tm > 0, jnp.logical_not(column)))
        def _():
            greet(place(tm, 0, last))

        @pl.when(both(column, tm > 0, plane != home))
        def _():
            greet(place(group * planes + home))

    def takes_from(s):
        return both(lead, sub != s, jnp.logical_or(sub > s, sub == 0))

    def gives_to(t):
        return both(lead, sub != t, jnp.logical_or(sub < t, t == 0))

    for s in range(n_sub):
        @pl.when(takes_from(s))
        def _():
            greet(place(sub_at=s))

    @pl.when(head)
    def _():
        for k in range(planes):
            if k != home:
                greet(place(group * planes + k))

        @pl.when(group > 0)
        def _():
            greet(place((group - 1) * planes + home))

    for load in loads[1:]:
        load.wait()
    weights = Weights(weight_ref, onto_ref, back_ref, bias_ref, amplitude_ref)
    weights.fill(weight_ref[...])
    start = start_ref[...]
    window = Window(weights, guess_ref[...], start)
    found = [stationary(k) for k in weights.hessians(window.curves, window.diagonal)]
    run_ref[...] = window_map(window, found)
    start_q, start_p = window.start_q, window.start_p

    count = jnp.where(jnp.logical_and(lead, jnp.logical_not(opening_chip)), 1, 0)
    count = count + jnp.where(other, 1, 0)
    count = count + jnp.where(lead, jnp.where(sub == 0, n_sub - 1, n_sub - sub), 0)
    count = count + jnp.where(jnp.logical_and(column, plane != home), 1, 0)
    count = count + jnp.where(head, jnp.where(group > 0, planes - 1, planes - 2), 0)
    count = count + jnp.where(jnp.logical_and(column, tm > 0), around - 1, 0)
    count = count + jnp.where(jnp.logical_and(head, group < n_groups - 1), 1, 0)

    @pl.when(jnp.logical_not(origin))
    def _():
        pl.semaphore_wait(barrier, count)

    entry, arrived, onward = 0, planes + 1, planes + 2

    @pl.when(origin)
    def _():
        upright_ref[...] = jnp.broadcast_to(stand(window.first), (state, state))

    for t in range(steps):
        kicks_ref[t, :, :state] = found[t]
    open_ref[...] = found[steps]
    offs_ref[0] = window.off_q
    offs_ref[1] = window.off_p
    rows_ref[0] = window.moved
    rows_ref[1] = window.landed
    plain = weights.hessians(window.curve_one, [curvature] * steps)
    for t in range(steps):
        kicks_ref[t, :, state:] = stationary(plain[t])

    to_lead = copy(run_ref, core_ref, pair_send, pair_recv, place(inner_at=last))
    to_other = copy(pre_ref, pre_ref, pair_send, pair_recv, place(inner_at=0))
    to_head = copy(
        majors_ref.at[plane], majors_ref.at[plane], column_send, majors_recv,
        place(group * planes + home),
    )

    def to_sub(t):
        return copy(
            subs_ref.at[sub], subs_ref.at[sub], subs_send, subs_recv, place(sub_at=t)
        )

    def some_subs(count):
        part_of = subs_ref.at[pl.ds(0, count)]
        return copy(part_of, part_of, subs_send, subs_recv, place())

    given = jnp.where(sub == 0, n_sub - 1, n_sub - sub)
    taken = jnp.where(sub == 0, n_sub - 1, sub)

    @pl.when(jnp.logical_and(other, jnp.logical_not(origin)))
    def _():
        to_lead.start()

    @pl.when(lead)
    def _():
        @pl.when(opening_chip)
        def _():
            subs_ref[sub] = run_ref[...]

        @pl.when(jnp.logical_not(opening_chip))
        def _():
            to_lead.wait_recv()
            subs_ref[sub] = compose(core_ref[...], run_ref[...])

        for t in range(n_sub):
            @pl.when(gives_to(t))
            def _():
                to_sub(t).start()

        for k in range(1, n_sub):
            @pl.when(taken == k)
            def _():
                some_subs(k).wait_recv()

        pre_ref[...] = identity(state)
        for k in range(n_sub - 1):
            @pl.when(k < sub)
            def _():
                pre_ref[...] = compose(pre_ref[...], subs_ref[k])

        @pl.when(jnp.logical_not(opening_chip))
        def _():
            to_other.start()
            run_ref[...] = compose(pre_ref[...], core_ref[...])

        @pl.when(opening_chip)
        def _():
            run_ref[...] = identity(state)

        @pl.when(sub == 0)
        def _():
            majors_ref[plane] = chain([subs_ref[k] for k in range(n_sub)])

            @pl.when(plane != home)
            def _():
                to_head.start()

            @pl.when(plane == home)
            def _():
                others = majors_ref.at[pl.ds(0, planes - 1)]
                copy(others, others, column_send, majors_recv, place()).wait_recv()
                ahead_ref[0] = majors_ref[0]
                for k in range(1, planes):
                    ahead_ref[k] = compose(ahead_ref[k - 1], majors_ref[k])

    @pl.when(other)
    def _():
        @pl.when(origin)
        def _():
            run_ref[...] = identity(state)

        @pl.when(jnp.logical_not(origin))
        def _():
            to_lead.wait_send()
            to_other.wait_recv()
            run_ref[...] = pre_ref[...]

    coords, momenta = twice(run_ref[...])
    coords, momenta = with_tail(coords, -start_q), with_tail(momenta, -start_p)
    momenta = momenta - kick(coords, open_ref[...])

    def advance(t, carry):
        coords, momenta = carry
        coords = coords + step_size * momenta
        pair = kick(coords, kicks_ref[t])
        row = pl.ds(t, 1)
        maps_ref[t] = join(
            with_tail(coords, rows_ref[0, row, :]),
            with_tail(momenta - pair[:, state:], rows_ref[1, row, :]),
        )
        return (
            with_tail(coords, offs_ref[0, row, :]),
            with_tail(momenta - pair[:, :state], offs_ref[1, row, :]),
        )

    lax.fori_loop(0, steps - 1, advance, (coords, momenta))

    to_next = copy(
        vector_ref.at[onward], vector_ref.at[entry], column_send, state_recv,
        place((group + 1) * planes + home),
    )

    def to_plane(k):
        return copy(
            vector_ref.at[k], vector_ref.at[arrived], spread_send, state_recv,
            place(group * planes + k),
        )

    def to_device(at):
        return copy(
            vector_ref.at[arrived], vector_ref.at[arrived], spread_send, state_recv,
            place(tm, at // n_inner, at % n_inner),
        )

    def spread():
        for at in range(around):
            if at != last:
                to_device(at).start()

    def stand_at(slot):
        upright_ref[...] = jnp.broadcast_to(stand(vector_ref[slot]), (state, state))

    @pl.when(starts)
    def _():
        copy(guess_ref, raw_ref, spread_send, state_recv, place(0, 0, 0)).wait_recv()
        left = left_state(weights, raw_ref[...], start_ref[...])
        upright_ref[...] = jnp.broadcast_to(left, (state, state))

    @pl.when(head)
    def _():
        @pl.when(group > 0)
        def _():
            to_next.wait_recv()
            stand_at(entry)

        for k in range(planes):
            slot = k + 1 if k + 1 < planes else onward
            vector_ref[arrived if slot == home else slot] = laid(upright_ref[...], ahead_ref[k])

        @pl.when(group < n_groups - 1)
        def _():
            to_next.start()

        for k in range(1, planes):
            if k != home:
                to_plane(k).start()

        @pl.when(group > 0)
        def _():
            to_plane(0).start()

        spread()
        stand_at(arrived)

    @pl.when(both(tm > 0, jnp.logical_not(head)))
    def _():
        to_device(0).wait_recv()

        @pl.when(column)
        def _():
            spread()

        stand_at(arrived)

    upright = upright_ref[...]
    for t in range(steps):
        ref = run_ref if t == 0 else maps_ref.at[t - 1]
        out_ref[t : t + 1, :] = laid(upright, ref)

    def spread_left(rows):
        sent = maps_ref.at[0, pl.ds(0, rows), :]
        copy(sent, sent, spread_send, state_recv, place()).wait_send()

    @pl.when(origin)
    def _():
        spread_left(around * steps)

    @pl.when(lead)
    def _():
        for k in range(1, n_sub):
            @pl.when(given == k)
            def _():
                some_subs(k).wait_send()

        @pl.when(jnp.logical_not(opening_chip))
        def _():
            to_other.wait_send()

        @pl.when(jnp.logical_and(column, plane != home))
        def _():
            to_head.wait_send()

    @pl.when(both(head, group > 0))
    def _():
        spread_left(planes + around - 2)

    @pl.when(both(head, group == 0))
    def _():
        spread_left(planes + around - 3)

    @pl.when(both(column, tm > 0, plane != home))
    def _():
        spread_left(around - 1)

    @pl.when(both(head, group < n_groups - 1))
    def _():
        to_next.wait_send()


def shards(sizes, guess, start, layer_weight, layer_bias, amplitude):
    n_tm, n_sub, n_inner = sizes
    steps, state = guess.shape
    rows = state + tail
    hidden = layer_bias.shape[0]
    vmem = pl.BlockSpec(memory_space=pltpu.VMEM)
    dma = pltpu.SemaphoreType.DMA
    return pl.pallas_call(
        functools.partial(kernel, sizes),
        out_shape=pltpu.VMEM((steps, state), f32),
        in_specs=[pl.BlockSpec(memory_space=pl.ANY)] * 5,
        out_specs=vmem,
        scratch_shapes=[
            pltpu.VMEM((steps, state), f32),
            pltpu.VMEM((1, state), f32),
            pltpu.VMEM((state // 2, hidden), f32),
            pltpu.VMEM((1, hidden), f32),
            pltpu.VMEM((1, hidden), f32),
            pltpu.VMEM((steps, 2 * state, 2 * state), bf16),
            pltpu.VMEM((2 * state, state), bf16),
            pltpu.VMEM((2, steps, state), f32),
            pltpu.VMEM((2, steps, state), f32),
            pltpu.VMEM((rows, state), f32),
            pltpu.VMEM((n_sub, rows, state), f32),
            pltpu.VMEM((planes, rows, state), f32),
            pltpu.VMEM((planes, rows, state), f32),
            pltpu.VMEM((rows, state), f32),
            pltpu.VMEM((rows, state), f32),
            pltpu.VMEM((3 + planes, 1, state), f32),
            pltpu.VMEM((steps, rows, state), f32),
            pltpu.VMEM((2 * state, hidden), bf16),
            pltpu.VMEM((hidden, 2 * state), bf16),
            pltpu.VMEM((steps, state), f32),
            pltpu.VMEM((state, state), f32),
            dma,
            dma,
            dma,
            dma,
            dma,
            dma,
            dma,
            dma,
            dma,
            dma,
        ],
        compiler_params=pltpu.CompilerParams(collective_id=0, has_side_effects=True),
    )(guess, start.reshape(1, -1), layer_weight.T, layer_bias.reshape(1, -1), amplitude.reshape(1, -1))


def solution(mesh):
    sizes = tuple(mesh.shape[name] for name in ("tm", "sub", "inner"))
    placed = (P(("parts", "tm", "sub", "inner"), None), P("parts"), P(), P(), P())
    return jax.shard_map(
        functools.partial(shards, sizes),
        mesh=mesh,
        in_specs=placed,
        out_specs=P(("parts", "tm", "sub", "inner"), None),
        check_vma=False,
    )
```
